32 devices in a mesh: rep: 1, r: 4 (over z), s: 8 (over x, y, core).
Axes of the slice: x: 2, y: 2, z: 4, core: 2. Of those that a mesh axis runs over, the one named last changes fastest.
Arguments:
- x: bfloat16 [32, 4096, 512], P(('rep', 'r', 's'))
- dy: bfloat16 [32, 4096, 512], P(('rep', 'r', 's'))
- w_gate: bfloat16 [2, 512, 1280], P(None, 's')
- w_up: bfloat16 [2, 512, 1280], P(None, 's')
- w_down: bfloat16 [2, 1280, 512], P(None, 's')
Outputs:
- output 1: bfloat16 [32, 4096, 512], P(('rep', 'r', 's'))
- output 2: bfloat16 [2, 512, 1280], P('rep', 's')
- output 3: bfloat16 [2, 512, 1280], P('rep', 's')
- output 4: bfloat16 [2, 1280, 512], P('rep', 's')
All inputs are finite; a program needn't handle non-finite values.
Results may differ from the reference program's by a relative error of at most 0.018.
Values are sent between devices in bfloat16 or wider.
A program may use at most 2 GiB of HBM per device.

```python
import jax
import jax.numpy as jnp
from jax import lax

SEQUENCES = 32
TOKENS = 4096
D = 512
FF = 1280
LAYERS = 2
NAMES = ("w_gate", "w_up", "w_down")
SHAPES = {"w_gate": (LAYERS, D, FF), "w_up": (LAYERS, D, FF), "w_down": (LAYERS, FF, D)}


def bump(key, n, height):
    away = (jnp.arange(n, dtype=jnp.int32) - jax.random.randint(key, (), 0, n, jnp.int32)) % n
    return jnp.where(away < n // 8, height, 1.0)


def together(key, own, strength):
    shared = jax.random.normal(key, own.shape[1:], jnp.float32)
    return (own + strength * shared) * lax.rsqrt(1 + strength * strength)


def setup_inputs(seed: int = 0, part: int = 0) -> dict:
    kx, kdy, ka, kb, kz, kf, kh, kl, *kw = jax.random.split(jax.random.key(seed), 8 + len(NAMES))
    kx, kdy, ka, kb = (jax.random.fold_in(k, part) for k in (kx, kdy, ka, kb))
    shape = (SEQUENCES, TOKENS, D)
    much_x, much_dy = jax.random.uniform(kz, (2,), jnp.float32, 0.0, 1.0)
    layers = 2.0 ** jax.random.uniform(kl, (LAYERS, 1, 1), jnp.float32, -1.0, 1.0)
    x = together(ka, jax.random.normal(kx, shape, jnp.float32), much_x) * bump(kf, D, 4.0)
    dy = together(kb, jax.random.normal(kdy, shape, jnp.float32), much_dy)
    drawn = {"x": x.astype(jnp.bfloat16), "dy": (dy * (SEQUENCES * TOKENS) ** -0.5).astype(jnp.bfloat16)}
    for key, name in zip(kw, NAMES, strict=True):
        w = jax.random.normal(key, SHAPES[name], jnp.float32) * SHAPES[name][1] ** -0.5
        drawn[name] = (w * {"w_gate": 1.0, "w_up": bump(kh, FF, 4.0), "w_down": layers}[name]).astype(jnp.bfloat16)
    return drawn


def matmul(a, w):
    return jnp.dot(a, w, preferred_element_type=jnp.float32).astype(jnp.bfloat16)


def normed(h):
    wide = h.astype(jnp.float32)
    scale = lax.rsqrt(jnp.mean(wide**2, -1, keepdims=True) + 1e-6)
    return (wide * scale).astype(jnp.bfloat16)


def layer(h, w):
    a = normed(h)
    gate = jnp.dot(a, w["w_gate"], preferred_element_type=jnp.float32)
    up = jnp.dot(a, w["w_up"], preferred_element_type=jnp.float32)
    return h + matmul((jax.nn.silu(gate) * up).astype(jnp.bfloat16), w["w_down"])


def stack(weights, h):
    return lax.scan(lambda h, w: (layer(h, w), None), h, weights)[0]


def reference(x, dy, w_gate, w_up, w_down):
    weights = dict(zip(NAMES, (w_gate, w_up, w_down), strict=True))

    def take(so_far, sequence):
        h, by_y = sequence
        _, back = jax.vjp(stack, weights, h)
        by_weights, by_h = back(by_y)
        return jax.tree.map(lambda total, term: total + term.astype(jnp.float32), so_far, by_weights), by_h

    none_yet = {name: jnp.zeros(w.shape, jnp.float32) for name, w in weights.items()}
    by_weights, by_x = lax.scan(take, none_yet, (x, dy))
    return (by_x, *(by_weights[name].astype(jnp.bfloat16) for name in NAMES))
```

```python
import functools

import jax
import jax.numpy as jnp
from jax import lax
from jax.experimental import pallas as pl
from jax.experimental.pallas import tpu as pltpu
from jax.sharding import PartitionSpec as P

MESH = pl.DeviceIdType.MESH
F32, BF16 = jnp.float32, jnp.bfloat16
W = 256
S, R = 8, 4


def dot(a, b, dims):
    return lax.dot_general(a, b, (dims, ((), ())), preferred_element_type=F32)


NN, NT = ((1,), (0,)), ((1,), (1,))


def mean_square(wide):
    return jnp.mean(wide * wide, axis=-1, keepdims=True) + 1e-6


def kernel(
    tokens, d, ff, tile, small,
    x_ref, dy_ref, wg_ref, wu_ref, wd_ref,
    dx_ref, og_ref, ou_ref, od_ref, keep_a, keep_at,
    WG, WU, WD, A, AT, H, DH, DG, DU, ACC,
    C, R1, O1, B2, R2, O2, B3, R3, B4, OGU, OD,
    in_sem, own_sem, keep_sem, gs_sem, gr_sem, fs_sem, fr_sem,
    s1_sem, r1_sem, s2_sem, r2_sem, s3_sem, r3_sem, s4_sem, r4_sem, rd_sem, out_sem, dx_sem,
):
    z, s = lax.axis_index("r"), lax.axis_index("s")
    core, yy, xx = s % 2, (s // 2) % 2, s // 4
    xy = s // 2
    chunks = ff // W
    rows_d, rows_f = d // S, ff // S

    def at(px, py, pc):
        return 4 * px + 2 * py + pc

    def to(sem_s, sem_r, src, dst, r, dev):
        return pltpu.make_async_remote_copy(
            src_ref=src, dst_ref=dst, send_sem=sem_s, recv_sem=sem_r,
            device_id={"r": r, "s": dev}, device_id_type=MESH)

    sib = at(xx, yy, 1 - core)
    others = (at(1 - xx, yy, core), at(xx, 1 - yy, core), at(1 - xx, 1 - yy, core))

    mats = ((wg_ref, WG, rows_d), (wu_ref, WU, rows_d), (wd_ref, WD, rows_f))

    def block(m, l, dev):
        _, full, rows = mats[m]
        return full.at[l, pl.ds(pl.multiple_of(dev * rows, rows), rows)]

    def spread(m, l):
        return [to(gs_sem.at[l, m, i], gr_sem.at[l, m, i], mats[m][0].at[l], block(m, l, s), z, dev)
                for i, dev in enumerate(others + (sib,))]

    def onward(m, l):
        return [to(fs_sem.at[l, m, i], fr_sem.at[l, m, i], block(m, l, dev), block(m, l, dev), z, sib)
                for i, dev in enumerate(others)]

    def own(m, l):
        return pltpu.make_async_copy(mats[m][0].at[l], block(m, l, s), own_sem.at[l, m])

    def forward(l, ms):
        for m in ms:
            first, second = spread(m, l), onward(m, l)
            for i in range(3):
                first[i].wait_recv()
                second[i].start()

    def arrived(l, ms):
        for m in ms:
            own(m, l).wait()
            spread(m, l)[3].wait_recv()
            for copy in onward(m, l):
                copy.wait_recv()

    for l in range(2):
        for m in range(3):
            for copy in spread(m, l):
                copy.start()
    tiles, few = tokens // tile, tokens // small

    def x_in(i):
        r = pl.ds(i * small, small)
        return (pltpu.make_async_copy(x_ref.at[0, r], H.at[r], in_sem.at[0, i]),
                pltpu.make_async_copy(dy_ref.at[0, r], DH.at[r], in_sem.at[1, i]))

    for i in range(few):
        for copy in x_in(i):
            copy.start()
    for l in range(2):
        for m in range(3):
            own(m, l).start()

    def enter(i, _):
        r = pl.ds(pl.multiple_of(i * small, small), small)
        pltpu.make_async_copy(x_ref.at[0, r], H.at[r], in_sem.at[0, i]).wait()
        pltpu.make_async_copy(dy_ref.at[0, r], DH.at[r], in_sem.at[1, i]).wait()
        wide = H[r, :].astype(F32)
        a = (wide * lax.rsqrt(mean_square(wide))).astype(BF16)
        A[r, :] = a
        AT[:, r] = a.T
        return 0

    lax.fori_loop(0, few, enter, 0)
    keep = (pltpu.make_async_copy(A, keep_a, keep_sem.at[0]), pltpu.make_async_copy(AT, keep_at, keep_sem.at[1]))
    for copy in keep:
        copy.start()

    def columns(c):
        return pl.ds(pl.multiple_of(c * W, W), W)

    forward(0, (0, 1))
    arrived(0, (0, 1))

    def gated(i, _):
        c, t = i // tiles, i % tiles
        r, cs = pl.ds(pl.multiple_of(t * tile, tile), tile), columns(c)
        a = A[r, :]
        g, u = dot(a, WG[0, :, cs], NN), dot(a, WU[0, :, cs], NN)
        DG[r, cs] = (g * (1.0 / (1.0 + jnp.exp(-g))) * u).astype(BF16)
        return 0

    lax.fori_loop(0, 2 * tiles, gated, 0)
    forward(0, (2,))
    lax.fori_loop(2 * tiles, chunks * tiles, gated, 0)
    arrived(0, (2,))
    for copy in keep:
        copy.wait()

    def down(i, _):
        r = pl.ds(pl.multiple_of(i * small, small), small)
        h = H[r, :].astype(F32) + dot(DG[r, :], WD[0], NN).astype(BF16).astype(F32)
        H[r, :] = h.astype(BF16)
        wide = h.astype(BF16).astype(F32)
        a = (wide * lax.rsqrt(mean_square(wide))).astype(BF16)
        A[r, :] = a
        AT[:, r] = a.T
        return 0

    lax.fori_loop(0, few // 2, down, 0)
    forward(1, (0, 1, 2))
    lax.fori_loop(few // 2, few, down, 0)
    arrived(1, (0, 1, 2))

    def first_hop(k):
        slot = k % 2
        return to(s1_sem.at[0], r1_sem.at[slot], C.at[1 - core], R1.at[slot], z, sib)

    def second_hop(k):
        slot = k % 2
        places = ((1 - xx) * 2 + yy, xx * 2 + 1 - yy, (1 - xx) * 2 + 1 - yy)
        return [to(s2_sem.at[i], r2_sem.at[slot, i], B2.at[places[i]], R2.at[slot, i], z, others[i]) for i in range(3)]

    def third_hop(k):
        slot = k % 2
        return [to(s3_sem.at[i], r3_sem.at[slot, i], B3.at[(z + 1 + i) % R], R3.at[slot, i], (z + 1 + i) % R, s)
                for i in range(3)]

    def spread_gu(l, c):
        return [to(s4_sem.at[i], r4_sem.at[l, c, i], B4.at[pl.ds(0, 2)],
                   OGU.at[l, :, pl.ds(pl.multiple_of(z * 16, 16), 16), columns(c)], (z + 1 + i) % R, s)
                for i in range(3)]

    def place_d(p, zz):
        return (pl.ds(pl.multiple_of((p % chunks) * 32 + (zz // 2) * 16, 16), 16),
                pl.ds(pl.multiple_of((zz % 2) * W, W), W))

    def spread_d(l, c, zz):
        p = S * c + s
        rows, cols = place_d(p, z)
        return to(s4_sem.at[3 + zz], rd_sem.at[l, p % chunks, z], B4.at[2], OD.at[l, rows, cols], zz, p // chunks)

    def each_d(c, fn):
        for zz in range(R):
            @pl.when(jnp.logical_not(jnp.logical_and((S * c + s) // chunks == s, z == zz)))
            def _(zz=zz):
                fn(zz)

    def wait_fourth(l, c):
        for copy in spread_gu(l, c):
            copy.wait_send()
        each_d(c, lambda zz: spread_d(l, c, zz).wait_send())

    def stage_1(l, c, k):
        first_hop(k).wait()
        mine = C.at[core]
        got = R1.at[k % 2]
        for i in range(4):
            total = mine[i].astype(F32) + got[i].astype(F32)
            B2[i] = total.astype(BF16)

            @pl.when(i == xy)
            def _(total=total):
                O1[...] = total

        for copy in second_hop(k):
            copy.start()

    def stage_2(l, c, k):
        for copy in second_hop(k):
            copy.wait()
        slot = k % 2
        for i in range(R):
            total = O1[i]
            for j in range(3):
                total = total + R2[slot, j, i].astype(F32)
            B3[i] = total.astype(BF16)

            @pl.when(i == z)
            def _(total=total):
                O2[...] = total

        for copy in third_hop(k):
            copy.start()

    def stage_3(l, c, k):
        for copy in third_hop(k):
            copy.wait()

        @pl.when(k > 0)
        def _():
            before = k - 1
            wait_fourth(1 - before // chunks, before % chunks)

        slot = k % 2
        total = O2[...]
        for j in range(3):
            total = total + R3[slot, j].astype(F32)
        total = total.astype(BF16)
        B4[...] = total
        OGU[l, :, pl.ds(pl.multiple_of(z * 16, 16), 16), columns(c)] = total[0:2]
        p = S * c + s

        @pl.when(p // chunks == s)
        def _():
            rows, cols = place_d(p, z)
            OD[l, rows, cols] = total[2]

        for copy in spread_gu(l, c):
            copy.start()
        each_d(c, lambda zz: spread_d(l, c, zz).start())

    def at_step(t, when, l, c, k):
        for stage, step in zip((stage_1, stage_2, stage_3), when):
            @pl.when(t == step)
            def _(stage=stage):
                stage(l, c, k)

    def layer(li, _):
        l = 1 - li

        def chunk(c, _):
            k = li * chunks + c
            cs = columns(c)

            def part(t, _):
                r = pl.ds(pl.multiple_of(t * tile, tile), tile)
                a = A[r, :]
                g, u = dot(a, WG[l, :, cs], NN), dot(a, WU[l, :, cs], NN)
                dz = dot(DH[r, :], WD[l, cs, :], NT).astype(BF16).astype(F32)
                gate = 1.0 / (1.0 + jnp.exp(-g))
                act = g * gate
                hidden = (act * u).astype(BF16)
                du = (dz * act).astype(BF16)
                dg = (dz * u * (gate + act * (1.0 - gate))).astype(BF16)
                DG[r, cs] = dg
                DU[r, cs] = du
                at_t = AT[:, r]
                new = (dot(at_t, dg, NN), dot(at_t, du, NN))
                low = dot(hidden, DH[r, :], ((0,), (0,)))

                @pl.when(t == 0)
                def _():
                    ACC[0], ACC[1] = new
                    ACC[2, pl.ds(0, W)] = low[:, :W]
                    ACC[2, pl.ds(W, W)] = low[:, W:]

                @pl.when(t > 0)
                def _():
                    ACC[0] += new[0]
                    ACC[1] += new[1]
                    ACC[2, pl.ds(0, W)] += low[:, :W]
                    ACC[2, pl.ds(W, W)] += low[:, W:]

                @pl.when(c > 0)
                def _():
                    at_step(t, (0, tiles - 2, tiles - 1), l, c - 1, k - 1)

                return 0

            lax.fori_loop(0, tiles, part, 0)
            for dev in range(S):
                for q in range(R):
                    to_block = C.at[dev % 2, dev // 2, q]
                    gu = pl.ds(rows_d * dev + 16 * q, 16)
                    to_block[0] = ACC[0, gu].astype(BF16)
                    to_block[1] = ACC[1, gu].astype(BF16)
                    to_block[2] = ACC[2, pl.ds((q % 2) * W + 32 * dev + 16 * (q // 2), 16)].astype(BF16)
            first_hop(k).start()
            return 0

        lax.fori_loop(0, chunks, chunk, 0)

        @pl.when(li == 0)
        def _():
            pltpu.make_async_copy(keep_a, A, keep_sem.at[0]).start()
            pltpu.make_async_copy(keep_at, AT, keep_sem.at[1]).start()

        def below(i, _):
            r = pl.ds(pl.multiple_of(i * small, small), small)
            da = dot(DG[r, :], WG[l], NT).astype(BF16).astype(F32) + dot(DU[r, :], WU[l], NT).astype(BF16).astype(F32)
            da = da.astype(BF16).astype(F32)
            wide = H[r, :].astype(F32)
            scale = lax.rsqrt(mean_square(wide))
            along = jnp.mean(da * wide, axis=-1, keepdims=True)
            by_h = (scale * da - wide * (scale * scale * scale * along)).astype(BF16)
            dh = (by_h.astype(F32) + DH[r, :].astype(F32)).astype(BF16)
            DH[r, :] = dh

            @pl.when(li == 0)
            def _():
                pltpu.make_async_copy(x_ref.at[0, r], H.at[r], in_sem.at[0, i]).start()

            @pl.when(li == 1)
            def _():
                pltpu.make_async_copy(DH.at[r], dx_ref.at[0, r], dx_sem.at[i]).start()

            at_step(i, (0, few // 2 - 1, few // 2 + 1), l, chunks - 1, li * chunks + chunks - 1)
            return 0

        lax.fori_loop(0, few, below, 0)

        @pl.when(li == 0)
        def _():
            pltpu.make_async_copy(keep_a, A, keep_sem.at[0]).wait()
            pltpu.make_async_copy(keep_at, AT, keep_sem.at[1]).wait()
            for i in range(few):
                x_in(i)[0].wait()

        return 0

    lax.fori_loop(0, 2, layer, 0)

    wait_fourth(0, chunks - 1)
    for l in range(2):
        for c in range(chunks):
            for copy in spread_gu(l, c):
                copy.wait_recv()
        for pos in range(chunks):
            p = s * chunks + pos
            for zz in range(R):
                @pl.when(jnp.logical_not(jnp.logical_and(p % S == s, z == zz)))
                def _(l=l, pos=pos, zz=zz):
                    rows, cols = place_d(pos, zz)
                    to(s4_sem.at[0], rd_sem.at[l, pos, zz], B4.at[2], OD.at[l, rows, cols], z, s).wait_recv()
    last = (pltpu.make_async_copy(OGU.at[:, 0], og_ref, out_sem.at[0]),
            pltpu.make_async_copy(OGU.at[:, 1], ou_ref, out_sem.at[1]),
            pltpu.make_async_copy(OD, od_ref, out_sem.at[2]))
    for copy in last:
        copy.start()
    for l in range(2):
        for m in range(3):
            for copy in spread(m, l) + onward(m, l):
                copy.wait_send()
    for i in range(few):
        r = pl.ds(i * small, small)
        pltpu.make_async_copy(DH.at[r], dx_ref.at[0, r], dx_sem.at[i]).wait()
    for copy in last:
        copy.wait()


def whole(tokens, d, ff):
    tile, small = min(1024, tokens // 4), min(512, tokens // 8)
    few = tokens // small
    chunks = ff // W
    dma = pltpu.SemaphoreType.DMA
    layers = 2
    shape = jax.ShapeDtypeStruct
    rows_d, rows_f = d // S, ff // S
    any_space = pl.BlockSpec(memory_space=pl.ANY)
    flops = 2 * tokens * d * ff * 19
    return pl.pallas_call(
        functools.partial(kernel, tokens, d, ff, tile, small),
        out_shape=(
            shape((1, tokens, d), BF16), shape((layers, rows_d, ff), BF16), shape((layers, rows_d, ff), BF16),
            shape((layers, rows_f, d), BF16), shape((tokens, d), BF16), shape((d, tokens), BF16)),
        in_specs=[any_space] * 5,
        out_specs=(any_space,) * 6,
        scratch_shapes=[
            pltpu.VMEM((layers, d, ff), BF16), pltpu.VMEM((layers, d, ff), BF16), pltpu.VMEM((layers, ff, d), BF16),
            pltpu.VMEM((tokens, d), BF16), pltpu.VMEM((d, tokens), BF16),
            pltpu.VMEM((tokens, d), BF16), pltpu.VMEM((tokens, d), BF16),
            pltpu.VMEM((tokens, ff), BF16), pltpu.VMEM((tokens, ff), BF16),
            pltpu.VMEM((3, d, W), F32),
            pltpu.VMEM((2, 4, R, 3, 16, W), BF16), pltpu.VMEM((2, 4, R, 3, 16, W), BF16),
            pltpu.VMEM((R, 3, 16, W), F32), pltpu.VMEM((4, R, 3, 16, W), BF16),
            pltpu.VMEM((2, 3, R, 3, 16, W), BF16), pltpu.VMEM((3, 16, W), F32),
            pltpu.VMEM((R, 3, 16, W), BF16), pltpu.VMEM((2, 3, 3, 16, W), BF16),
            pltpu.VMEM((3, 16, W), BF16),
            pltpu.VMEM((layers, 2, rows_d, ff), BF16), pltpu.VMEM((layers, rows_f, d), BF16),
            dma((2, few)), dma((layers, 3)), dma((2,)),
            dma((layers, 3, 4)), dma((layers, 3, 4)), dma((layers, 3, 3)), dma((layers, 3, 3)),
            dma((1,)), dma((2,)), dma((3,)), dma((2, 3)), dma((3,)), dma((2, 3)),
            dma((7,)), dma((layers, chunks, 3)), dma((layers, chunks, R)), dma((3,)), dma((few,)),
        ],
        compiler_params=pltpu.CompilerParams(has_side_effects=True, vmem_limit_bytes=67_043_328),
        cost_estimate=pl.CostEstimate(flops=flops, bytes_accessed=4 * tokens * d * 2, transcendentals=0),
        name="stack",
    )


def solution(mesh):
    def step(x, dy, w_gate, w_up, w_down):
        _, tokens, d = x.shape
        ff = w_gate.shape[2]
        return whole(tokens, d, ff)(x, dy, w_gate, w_up, w_down)[:4]

    states, cut = P(("rep", "r", "s"), None, None), P(None, "s", None)
    return jax.shard_map(
        step,
        mesh=mesh,
        in_specs=(states, states) + (cut,) * 3,
        out_specs=(states,) + (P("rep", "s", None),) * 3,
        check_vma=False,
    )
```

```python
import functools

import jax
import jax.numpy as jnp
from jax import lax
from jax.experimental import pallas as pl
from jax.experimental.pallas import tpu as pltpu
from jax.sharding import PartitionSpec as P

MESH = pl.DeviceIdType.MESH
F32, BF16 = jnp.float32, jnp.bfloat16
W = 256
S, R = 8, 4


def dot(a, b, dims):
    return lax.dot_general(a, b, (dims, ((), ())), preferred_element_type=F32)


NN, NT = ((1,), (0,)), ((1,), (1,))


def mean_square(wide):
    return jnp.mean(wide * wide, axis=-1, keepdims=True) + 1e-6


def kernel(
    tokens, d, ff, tile, small,
    x_ref, dy_ref, wg_ref, wu_ref, wd_ref,
    dx_ref, og_ref, ou_ref, od_ref, keep_a, keep_at,
    WG, WU, WD, A, AT, H, DH, DG, DU, Z,
    C, R1, O1, B2, R2, O2, B3, R3, B4, OGU, OD,
    in_sem, own_sem, keep_sem, gs_sem, gr_sem, fs_sem, fr_sem,
    s1_sem, r1_sem, s2_sem, r2_sem, s3_sem, r3_sem, s4_sem, r4_sem, rd_sem, out_sem, dx_sem,
):
    z, s = lax.axis_index("r"), lax.axis_index("s")
    core, yy, xx = s % 2, (s // 2) % 2, s // 4
    xy = s // 2
    chunks = ff // W
    rows_d, rows_f = d // S, ff // S

    def at(px, py, pc):
        return 4 * px + 2 * py + pc

    def to(sem_s, sem_r, src, dst, r, dev):
        return pltpu.make_async_remote_copy(
            src_ref=src, dst_ref=dst, send_sem=sem_s, recv_sem=sem_r,
            device_id={"r": r, "s": dev}, device_id_type=MESH)

    sib = at(xx, yy, 1 - core)
    others = (at(1 - xx, yy, core), at(xx, 1 - yy, core), at(1 - xx, 1 - yy, core))

    mats = ((wg_ref, WG, rows_d), (wu_ref, WU, rows_d), (wd_ref, WD, rows_f))

    def columns(c):
        return pl.ds(pl.multiple_of(c * W, W), W)

    def piece(l, m, c, dev):
        _, full, rows = mats[m]
        r = pl.ds(pl.multiple_of(dev * rows, rows), rows)
        return full.at[l, r] if m == 2 else full.at[l, r, columns(c)]

    def mine(l, m, c):
        return mats[m][0].at[l] if m == 2 else mats[m][0].at[l, :, columns(c)]

    def spread(l, m, c, i):
        return to(gs_sem.at[l, m, c, i], gr_sem.at[l, m, c, i], mine(l, m, c), piece(l, m, c, s), z, (others + (sib,))[i])

    def onward(l, m, c, i):
        block = piece(l, m, c, others[i])
        return to(fs_sem.at[l, m, c, i], fr_sem.at[l, m, c, i], block, block, z, sib)

    def own(l, m):
        rows = mats[m][2]
        return pltpu.make_async_copy(
            mats[m][0].at[l], mats[m][1].at[l, pl.ds(pl.multiple_of(s * rows, rows), rows)], own_sem.at[l, m])

    def send(l, ms, c):
        for m in ms:
            for i in range(4):
                spread(l, m, c, i).start()

    def forward(l, ms, c):
        for m in ms:
            for i in range(3):
                spread(l, m, c, i).wait_recv()
                onward(l, m, c, i).start()

    def arrived(l, ms, c):
        for m in ms:
            spread(l, m, c, 3).wait_recv()
            for i in range(3):
                onward(l, m, c, i).wait_recv()

    def sent(l, ms, c):
        for m in ms:
            for i in range(4):
                spread(l, m, c, i).wait_send()
            for i in range(3):
                onward(l, m, c, i).wait_send()

    GU, DOWN = (0, 1), (2,)
    barrier = pltpu.get_barrier_semaphore()
    here = z * S + s

    def greet(i, _):
        there = (here + i) % (R * S)
        pl.semaphore_signal(barrier, inc=1, device_id={"r": there // S, "s": there % S}, device_id_type=MESH)
        return 0

    lax.fori_loop(1, R * S, greet, 0)
    tiles, few = tokens // tile, tokens // small
    fine = small // 2
    down_parts = tokens // fine

    def x_in(i):
        r = pl.ds(i * small, small)
        return (pltpu.make_async_copy(x_ref.at[0, r], H.at[r], in_sem.at[0, i]),
                pltpu.make_async_copy(dy_ref.at[0, r], DH.at[r], in_sem.at[1, i]))

    for i in range(few):
        for copy in x_in(i):
            copy.start()
    for l in range(2):
        for m in range(3):
            own(l, m).start()

    def enter(i, _):
        r = pl.ds(pl.multiple_of(i * small, small), small)
        pltpu.make_async_copy(x_ref.at[0, r], H.at[r], in_sem.at[0, i]).wait()
        wide = H[r, :].astype(F32)
        a = (wide * lax.rsqrt(mean_square(wide))).astype(BF16)
        A[r, :] = a
        AT[:, r] = a.T
        return 0

    lax.fori_loop(0, few, enter, 0)
    pl.semaphore_wait(barrier, R * S - 1)
    for c in range(chunks):
        send(0, GU, c)
    send(0, DOWN, 0)
    keep = (pltpu.make_async_copy(A, keep_a, keep_sem.at[0]), pltpu.make_async_copy(AT, keep_at, keep_sem.at[1]))
    for copy in keep:
        copy.start()

    forward(0, GU, 0)
    send(1, DOWN, 0)
    for c in range(chunks):
        send(1, GU, c)
    for l in range(2):
        for m in range(3):
            own(l, m).wait()

    def gated(c, _):
        cs = columns(c)
        arrived(0, GU, c)
        for t in range(tiles):
            if t == tiles // 2:
                @pl.when(c < chunks - 1)
                def _():
                    forward(0, GU, c + 1)
            r = pl.ds(t * tile, tile)
            a = A[r, :]
            g, u = dot(a, WG[0, :, cs], NN), dot(a, WU[0, :, cs], NN)
            DG[r, cs] = (g * (1.0 / (1.0 + jnp.exp(-g))) * u).astype(BF16)
        return 0

    lax.fori_loop(0, chunks, gated, 0)
    forward(0, DOWN, 0)
    for i in range(few):
        x_in(i)[1].wait()
    arrived(0, DOWN, 0)
    for copy in keep:
        copy.wait()

    def down(i, _):
        for q in range(down_parts // 2):
            r = pl.ds(pl.multiple_of((i * (down_parts // 2) + q) * fine, fine), fine)
            h = (H[r, :].astype(F32) + dot(DG[r, :], WD[0], NN).astype(BF16).astype(F32)).astype(BF16)
            H[r, :] = h
            wide = h.astype(F32)
            a = (wide * lax.rsqrt(mean_square(wide))).astype(BF16)
            A[r, :] = a
            AT[:, r] = a.T

        @pl.when(i == 0)
        def _():
            forward(1, DOWN, 0)

        return 0

    lax.fori_loop(0, 2, down, 0)
    forward(1, GU, 0)
    arrived(1, DOWN, 0)

    def first_hop(k):
        slot = k % 2
        return to(s1_sem.at[0], r1_sem.at[slot], C.at[1 - core], R1.at[slot], z, sib)

    def second_hop(k):
        slot = k % 2
        places = ((1 - xx) * 2 + yy, xx * 2 + 1 - yy, (1 - xx) * 2 + 1 - yy)
        return [to(s2_sem.at[i], r2_sem.at[slot, i], B2.at[places[i]], R2.at[slot, i], z, others[i]) for i in range(3)]

    def third_hop(k):
        slot = k % 2
        return [to(s3_sem.at[i], r3_sem.at[slot, i], B3.at[(z + 1 + i) % R], R3.at[slot, i], (z + 1 + i) % R, s)
                for i in range(3)]

    def spread_gu(l, c):
        return [to(s4_sem.at[i], r4_sem.at[l, c, i], B4.at[pl.ds(0, 2)],
                   OGU.at[l, :, pl.ds(pl.multiple_of(z * 16, 16), 16), columns(c)], (z + 1 + i) % R, s)
                for i in range(3)]

    def place_d(p, zz):
        return (pl.ds(pl.multiple_of((p % chunks) * 32 + (zz // 2) * 16, 16), 16),
                pl.ds(pl.multiple_of((zz % 2) * W, W), W))

    def spread_d(l, c, zz):
        p = S * c + s
        rows, cols = place_d(p, z)
        return to(s4_sem.at[3 + zz], rd_sem.at[l, p % chunks, z], B4.at[2], OD.at[l, rows, cols], zz, p // chunks)

    def each_d(c, fn):
        for zz in range(R):
            @pl.when(jnp.logical_not(jnp.logical_and((S * c + s) // chunks == s, z == zz)))
            def _(zz=zz):
                fn(zz)

    def wait_fourth(l, c):
        for copy in spread_gu(l, c):
            copy.wait_send()
        each_d(c, lambda zz: spread_d(l, c, zz).wait_send())

    def stage_1(l, c, k):
        first_hop(k).wait()
        kept = C.at[core]
        got = R1.at[k % 2]
        for i in range(4):
            total = kept[i].astype(F32) + got[i].astype(F32)
            B2[i] = total.astype(BF16)

            @pl.when(i == xy)
            def _(total=total):
                O1[...] = total

        for copy in second_hop(k):
            copy.start()

    def stage_2(l, c, k):
        for copy in second_hop(k):
            copy.wait()
        slot = k % 2
        for i in range(R):
            total = O1[i]
            for j in range(3):
                total = total + R2[slot, j, i].astype(F32)
            B3[i] = total.astype(BF16)

            @pl.when(i == z)
            def _(total=total):
                O2[...] = total

        for copy in third_hop(k):
            copy.start()

    def stage_3(l, c, k):
        for copy in third_hop(k):
            copy.wait()

        @pl.when(k > 0)
        def _():
            before = k - 1
            wait_fourth(1 - before // chunks, before % chunks)

        slot = k % 2
        total = O2[...]
        for j in range(3):
            total = total + R3[slot, j].astype(F32)
        total = total.astype(BF16)
        B4[...] = total
        OGU[l, :, pl.ds(pl.multiple_of(z * 16, 16), 16), columns(c)] = total[0:2]
        p = S * c + s

        @pl.when(p // chunks == s)
        def _():
            rows, cols = place_d(p, z)
            OD[l, rows, cols] = total[2]

        for copy in spread_gu(l, c):
            copy.start()
        each_d(c, lambda zz: spread_d(l, c, zz).start())

    def layer(li, _):
        l = 1 - li

        def chunk(c, _):
            k = li * chunks + c
            cs = columns(c)

            @pl.when(li == 0)
            def _():
                arrived(1, GU, c)

            for t in range(tiles):
                r = pl.ds(t * tile, tile)
                a = A[r, :]
                g, u = dot(a, WG[l, :, cs], NN), dot(a, WU[l, :, cs], NN)
                dz = dot(DH[r, :], WD[l, cs, :], NT).astype(BF16).astype(F32)
                gate = 1.0 / (1.0 + jnp.exp(-g))
                act = g * gate
                Z[r, :] = (act * u).astype(BF16)
                DU[r, cs] = (dz * act).astype(BF16)
                DG[r, cs] = (dz * u * (gate + act * (1.0 - gate))).astype(BF16)

            @pl.when(jnp.logical_and(li == 0, c < chunks - 1))
            def _():
                forward(1, GU, c + 1)

            for back, stage in ((3, stage_3), (2, stage_2), (1, stage_1)):
                @pl.when(c >= back)
                def _(back=back, stage=stage):
                    stage(l, c - back, k - back)

            by_gate = dot(AT[...], DG[:, cs], NN).astype(BF16)
            by_up = dot(AT[...], DU[:, cs], NN).astype(BF16)
            by_down = dot(Z[...], DH[...], ((0,), (0,))).astype(BF16)
            for dev in range(S):
                for q in range(R):
                    to_block = C.at[dev % 2, dev // 2, q]
                    top = rows_d * dev + 16 * q
                    to_block[0] = by_gate[top:top + 16]
                    to_block[1] = by_up[top:top + 16]
                    top = 32 * dev + 16 * (q // 2)
                    to_block[2] = by_down[top:top + 16, (q % 2) * W:(q % 2) * W + W]
            first_hop(k).start()
            return 0

        lax.fori_loop(0, chunks, chunk, 0)

        @pl.when(li == 0)
        def _():
            pltpu.make_async_copy(keep_a, A, keep_sem.at[0]).start()
            pltpu.make_async_copy(keep_at, AT, keep_sem.at[1]).start()

        def below(i, _):
            r = pl.ds(pl.multiple_of(i * small, small), small)
            for q in range(2):
                r2 = pl.ds(pl.multiple_of(i * small + q * fine, fine), fine)
                da = (dot(DG[r2, :], WG[l], NT).astype(BF16).astype(F32)
                      + dot(DU[r2, :], WU[l], NT).astype(BF16).astype(F32)).astype(BF16).astype(F32)
                wide = H[r2, :].astype(F32)
                scale = lax.rsqrt(mean_square(wide))
                along = jnp.mean(da * wide, axis=-1, keepdims=True)
                by_h = (scale * da - wide * (scale * scale * scale * along)).astype(BF16)
                DH[r2, :] = (by_h.astype(F32) + DH[r2, :].astype(F32)).astype(BF16)

            @pl.when(li == 0)
            def _():
                pltpu.make_async_copy(x_ref.at[0, r], H.at[r], in_sem.at[0, i]).start()

            @pl.when(li == 1)
            def _():
                pltpu.make_async_copy(DH.at[r], dx_ref.at[0, r], dx_sem.at[i]).start()

            k = li * chunks + chunks - 1
            for step, stage, back in ((0, stage_3, 2), (0, stage_2, 1), (0, stage_1, 0), (3, stage_3, 1), (3, stage_2, 0), (5, stage_3, 0)):
                @pl.when(i == step * few // 8)
                def _(stage=stage, back=back):
                    stage(l, chunks - 1 - back, k - back)

            return 0

        lax.fori_loop(0, few, below, 0)

        @pl.when(li == 0)
        def _():
            pltpu.make_async_copy(keep_a, A, keep_sem.at[0]).wait()
            pltpu.make_async_copy(keep_at, AT, keep_sem.at[1]).wait()
            for i in range(few):
                x_in(i)[0].wait()

        return 0

    lax.fori_loop(0, 2, layer, 0)

    wait_fourth(0, chunks - 1)
    for l in range(2):
        for c in range(chunks):
            for copy in spread_gu(l, c):
                copy.wait_recv()
        for pos in range(chunks):
            p = s * chunks + pos
            for zz in range(R):
                @pl.when(jnp.logical_not(jnp.logical_and(p % S == s, z == zz)))
                def _(l=l, pos=pos, zz=zz):
                    rows, cols = place_d(pos, zz)
                    to(s4_sem.at[0], rd_sem.at[l, pos, zz], B4.at[2], OD.at[l, rows, cols], z, s).wait_recv()
    last = (pltpu.make_async_copy(OGU.at[:, 0], og_ref, out_sem.at[0]),
            pltpu.make_async_copy(OGU.at[:, 1], ou_ref, out_sem.at[1]),
            pltpu.make_async_copy(OD, od_ref, out_sem.at[2]))
    for copy in last:
        copy.start()
    for l in range(2):
        sent(l, DOWN, 0)

        def all_sent(c, _, l=l):
            sent(l, GU, c)
            return 0

        lax.fori_loop(0, chunks, all_sent, 0)
    for i in range(few):
        r = pl.ds(i * small, small)
        pltpu.make_async_copy(DH.at[r], dx_ref.at[0, r], dx_sem.at[i]).wait()
    for copy in last:
        copy.wait()


def whole(tokens, d, ff):
    tile, small = min(1024, tokens // 4), min(512, tokens // 8)
    few = tokens // small
    chunks = ff // W
    dma = pltpu.SemaphoreType.DMA
    layers = 2
    shape = jax.ShapeDtypeStruct
    rows_d, rows_f = d // S, ff // S
    any_space = pl.BlockSpec(memory_space=pl.ANY)
    flops = 2 * tokens * d * ff * 19
    return pl.pallas_call(
        functools.partial(kernel, tokens, d, ff, tile, small),
        out_shape=(
            shape((1, tokens, d), BF16), shape((layers, rows_d, ff), BF16), shape((layers, rows_d, ff), BF16),
            shape((layers, rows_f, d), BF16), shape((tokens, d), BF16), shape((d, tokens), BF16)),
        in_specs=[any_space] * 5,
        out_specs=(any_space,) * 6,
        scratch_shapes=[
            pltpu.VMEM((layers, d, ff), BF16), pltpu.VMEM((layers, d, ff), BF16), pltpu.VMEM((layers, ff, d), BF16),
            pltpu.VMEM((tokens, d), BF16), pltpu.VMEM((d, tokens), BF16),
            pltpu.VMEM((tokens, d), BF16), pltpu.VMEM((tokens, d), BF16),
            pltpu.VMEM((tokens, ff), BF16), pltpu.VMEM((tokens, ff), BF16),
            pltpu.VMEM((tokens, W), BF16),
            pltpu.VMEM((2, 4, R, 3, 16, W), BF16), pltpu.VMEM((2, 4, R, 3, 16, W), BF16),
            pltpu.VMEM((R, 3, 16, W), F32), pltpu.VMEM((4, R, 3, 16, W), BF16),
            pltpu.VMEM((2, 3, R, 3, 16, W), BF16), pltpu.VMEM((3, 16, W), F32),
            pltpu.VMEM((R, 3, 16, W), BF16), pltpu.VMEM((2, 3, 3, 16, W), BF16),
            pltpu.VMEM((3, 16, W), BF16),
            pltpu.VMEM((layers, 2, rows_d, ff), BF16), pltpu.VMEM((layers, rows_f, d), BF16),
            dma((2, few)), dma((layers, 3)), dma((2,)),
            dma((layers, 3, chunks, 4)), dma((layers, 3, chunks, 4)), dma((layers, 3, chunks, 3)), dma((layers, 3, chunks, 3)),
            dma((1,)), dma((2,)), dma((3,)), dma((2, 3)), dma((3,)), dma((2, 3)),
            dma((7,)), dma((layers, chunks, 3)), dma((layers, chunks, R)), dma((3,)), dma((few,)),
        ],
        compiler_params=pltpu.CompilerParams(has_side_effects=True, collective_id=0, vmem_limit_bytes=67_043_328),
        cost_estimate=pl.CostEstimate(flops=flops, bytes_accessed=4 * tokens * d * 2, transcendentals=0),
        name="stack",
    )


def solution(mesh):
    def step(x, dy, w_gate, w_up, w_down):
        _, tokens, d = x.shape
        ff = w_gate.shape[2]
        return whole(tokens, d, ff)(x, dy, w_gate, w_up, w_down)[:4]

    states, cut = P(("rep", "r", "s"), None, None), P(None, "s", None)
    return jax.shard_map(
        step,
        mesh=mesh,
        in_specs=(states, states) + (cut,) * 3,
        out_specs=(states,) + (P("rep", "s", None),) * 3,
        check_vma=False,
    )
```

```python
import functools

import jax
import jax.numpy as jnp
from jax import lax
from jax.experimental import pallas as pl
from jax.experimental.pallas import tpu as pltpu
from jax.sharding import PartitionSpec as P

MESH = pl.DeviceIdType.MESH
F32, BF16 = jnp.float32, jnp.bfloat16
W = 256
S, R = 8, 4


def dot(a, b, dims):
    return lax.dot_general(a, b, (dims, ((), ())), preferred_element_type=F32)


NN, NT = ((1,), (0,)), ((1,), (1,))


def mean_square(wide):
    return jnp.mean(wide * wide, axis=-1, keepdims=True) + 1e-6


def kernel(
    tokens, d, ff, tile, small,
    x_ref, dy_ref, wg_ref, wu_ref, wd_ref,
    dx_ref, og_ref, ou_ref, od_ref, keep_a, keep_at, keep_f, keep_z,
    WG, WU, WD, A, AT, H, DH, DG, DU, Z, F,
    C, R1, O1, B2, R2, O2, B3, R3, B4, OGU, OD,
    in_sem, own_sem, keep_sem, gs_sem, gr_sem, fs_sem, fr_sem,
    s1_sem, r1_sem, s2_sem, r2_sem, s3_sem, r3_sem, s4_sem, r4_sem, rd_sem, out_sem, dx_sem, f_sem, z_sem,
):
    z, s = lax.axis_index("r"), lax.axis_index("s")
    core, yy, xx = s % 2, (s // 2) % 2, s // 4
    xy = s // 2
    chunks = ff // W
    rows_d, rows_f = d // S, ff // S

    def at(px, py, pc):
        return 4 * px + 2 * py + pc

    def to(sem_s, sem_r, src, dst, r, dev):
        return pltpu.make_async_remote_copy(
            src_ref=src, dst_ref=dst, send_sem=sem_s, recv_sem=sem_r,
            device_id={"r": r, "s": dev}, device_id_type=MESH)

    sib = at(xx, yy, 1 - core)
    others = (at(1 - xx, yy, core), at(xx, 1 - yy, core), at(1 - xx, 1 - yy, core))

    mats = ((wg_ref, WG, rows_d), (wu_ref, WU, rows_d), (wd_ref, WD, rows_f))

    def columns(c):
        return pl.ds(pl.multiple_of(c * W, W), W)

    def piece(l, m, c, dev):
        _, full, rows = mats[m]
        r = pl.ds(pl.multiple_of(dev * rows, rows), rows)
        return full.at[l, r] if m == 2 else full.at[l, r, columns(c)]

    def mine(l, m, c):
        return mats[m][0].at[l] if m == 2 else mats[m][0].at[l, :, columns(c)]

    def spread(l, m, c, i):
        return to(gs_sem.at[l, m, c, i], gr_sem.at[l, m, c, i], mine(l, m, c), piece(l, m, c, s), z, (others + (sib,))[i])

    def onward(l, m, c, i):
        block = piece(l, m, c, others[i])
        return to(fs_sem.at[l, m, c, i], fr_sem.at[l, m, c, i], block, block, z, sib)

    def own(l, m):
        rows = mats[m][2]
        return pltpu.make_async_copy(
            mats[m][0].at[l], mats[m][1].at[l, pl.ds(pl.multiple_of(s * rows, rows), rows)], own_sem.at[l, m])

    def send(l, ms, c):
        for m in ms:
            for i in range(4):
                spread(l, m, c, i).start()

    def forward(l, ms, c):
        for m in ms:
            for i in range(3):
                spread(l, m, c, i).wait_recv()
                onward(l, m, c, i).start()

    def arrived(l, ms, c):
        for m in ms:
            spread(l, m, c, 3).wait_recv()
            for i in range(3):
                onward(l, m, c, i).wait_recv()

    def sent(l, ms, c):
        for m in ms:
            for i in range(4):
                spread(l, m, c, i).wait_send()
            for i in range(3):
                onward(l, m, c, i).wait_send()

    GU, DOWN = (0, 1), (2,)
    barrier = pltpu.get_barrier_semaphore()
    here = z * S + s

    def greet(i, _):
        there = (here + i) % (R * S)
        pl.semaphore_signal(barrier, inc=1, device_id={"r": there // S, "s": there % S}, device_id_type=MESH)
        return 0

    lax.fori_loop(1, R * S, greet, 0)
    tiles, few = tokens // tile, tokens // small
    fine = small // 2
    down_parts = tokens // fine

    def x_in(i):
        r = pl.ds(i * small, small)
        return (pltpu.make_async_copy(x_ref.at[0, r], H.at[r], in_sem.at[0, i]),
                pltpu.make_async_copy(dy_ref.at[0, r], DH.at[r], in_sem.at[1, i]))

    for i in range(few):
        for copy in x_in(i):
            copy.start()
    for l in range(2):
        for m in range(3):
            own(l, m).start()

    def enter(i, _):
        r = pl.ds(pl.multiple_of(i * small, small), small)
        pltpu.make_async_copy(x_ref.at[0, r], H.at[r], in_sem.at[0, i]).wait()
        wide = H[r, :].astype(F32)
        a = (wide * lax.rsqrt(mean_square(wide))).astype(BF16)
        A[r, :] = a
        AT[:, r] = a.T
        return 0

    lax.fori_loop(0, few, enter, 0)
    pl.semaphore_wait(barrier, R * S - 1)
    for c in range(chunks):
        send(0, GU, c)
    send(0, DOWN, 0)
    keep = (pltpu.make_async_copy(A, keep_a, keep_sem.at[0]), pltpu.make_async_copy(AT, keep_at, keep_sem.at[1]))
    for copy in keep:
        copy.start()

    forward(0, GU, 0)
    send(1, DOWN, 0)
    for c in range(chunks):
        send(1, GU, c)
    for l in range(2):
        for m in range(3):
            own(l, m).wait()

    def factors_out(c, t):
        r = pl.ds(pl.multiple_of(t * tile, tile), tile)
        return pltpu.make_async_copy(F.at[:, r], keep_f.at[c, :, r], f_sem.at[t])

    def factors_in(c, t):
        r = pl.ds(t * tile, tile)
        return pltpu.make_async_copy(keep_f.at[c, :, r], F.at[:, r], f_sem.at[t])

    def hidden_in(c):
        return pltpu.make_async_copy(keep_z.at[:, columns(c)], Z, z_sem.at[0])

    def gated(i, _):
        c, t = i // tiles, i % tiles
        r, cs = pl.ds(pl.multiple_of(t * tile, tile), tile), columns(c)

        @pl.when(t == 0)
        def _():
            arrived(0, GU, c)

        @pl.when(c > 0)
        def _():
            factors_out(c - 1, t).wait()

        a = A[r, :]
        g, u = dot(a, WG[0, :, cs], NN), dot(a, WU[0, :, cs], NN)
        gate = 1.0 / (1.0 + jnp.exp(-g))
        act = g * gate
        DG[r, cs] = (act * u).astype(BF16)
        F[0, r] = act
        F[1, r] = u * (gate + act * (1.0 - gate))
        factors_out(c, t).start()

        @pl.when(jnp.logical_and(t == 1, c < chunks - 1))
        def _():
            forward(0, GU, c + 1)

        return 0

    lax.fori_loop(0, chunks * tiles, gated, 0)
    all_hidden = pltpu.make_async_copy(DG, keep_z, z_sem.at[0])
    all_hidden.start()
    forward(0, DOWN, 0)
    for i in range(few):
        x_in(i)[1].wait()
    arrived(0, DOWN, 0)
    for copy in keep:
        copy.wait()

    def down(i, _):
        for q in range(down_parts // 2):
            r = pl.ds(pl.multiple_of((i * (down_parts // 2) + q) * fine, fine), fine)
            h = (H[r, :].astype(F32) + dot(DG[r, :], WD[0], NN).astype(BF16).astype(F32)).astype(BF16)
            H[r, :] = h
            wide = h.astype(F32)
            a = (wide * lax.rsqrt(mean_square(wide))).astype(BF16)
            A[r, :] = a
            AT[:, r] = a.T

        @pl.when(i == 0)
        def _():
            forward(1, DOWN, 0)

        return 0

    lax.fori_loop(0, 2, down, 0)
    forward(1, GU, 0)
    arrived(1, DOWN, 0)
    all_hidden.wait()
    for t in range(tiles):
        factors_out(chunks - 1, t).wait()

    def first_hop(k):
        slot = k % 2
        return to(s1_sem.at[0], r1_sem.at[slot], C.at[1 - core], R1.at[slot], z, sib)

    def second_hop(k):
        slot = k % 2
        places = ((1 - xx) * 2 + yy, xx * 2 + 1 - yy, (1 - xx) * 2 + 1 - yy)
        return [to(s2_sem.at[i], r2_sem.at[slot, i], B2.at[places[i]], R2.at[slot, i], z, others[i]) for i in range(3)]

    def third_hop(k):
        slot = k % 2
        return [to(s3_sem.at[i], r3_sem.at[slot, i], B3.at[(z + 1 + i) % R], R3.at[slot, i], (z + 1 + i) % R, s)
                for i in range(3)]

    def spread_gu(l, c):
        return [to(s4_sem.at[i], r4_sem.at[l, c, i], B4.at[pl.ds(0, 2)],
                   OGU.at[l, :, pl.ds(pl.multiple_of(z * 16, 16), 16), columns(c)], (z + 1 + i) % R, s)
                for i in range(3)]

    def place_d(p, zz):
        return (pl.ds(pl.multiple_of((p % chunks) * 32 + (zz // 2) * 16, 16), 16),
                pl.ds(pl.multiple_of((zz % 2) * W, W), W))

    def spread_d(l, c, zz):
        p = S * c + s
        rows, cols = place_d(p, z)
        return to(s4_sem.at[3 + zz], rd_sem.at[l, p % chunks, z], B4.at[2], OD.at[l, rows, cols], zz, p // chunks)

    def each_d(c, fn):
        for zz in range(R):
            @pl.when(jnp.logical_not(jnp.logical_and((S * c + s) // chunks == s, z == zz)))
            def _(zz=zz):
                fn(zz)

    def wait_fourth(l, c):
        for copy in spread_gu(l, c):
            copy.wait_send()
        each_d(c, lambda zz: spread_d(l, c, zz).wait_send())

    def stage_1(l, c, k):
        first_hop(k).wait()
        kept = C.at[core]
        got = R1.at[k % 2]
        for i in range(4):
            total = kept[i].astype(F32) + got[i].astype(F32)
            B2[i] = total.astype(BF16)

            @pl.when(i == xy)
            def _(total=total):
                O1[...] = total

        for copy in second_hop(k):
            copy.start()

    def stage_2(l, c, k):
        for copy in second_hop(k):
            copy.wait()
        slot = k % 2
        for i in range(R):
            total = O1[i]
            for j in range(3):
                total = total + R2[slot, j, i].astype(F32)
            B3[i] = total.astype(BF16)

            @pl.when(i == z)
            def _(total=total):
                O2[...] = total

        for copy in third_hop(k):
            copy.start()

    def stage_3(l, c, k):
        for copy in third_hop(k):
            copy.wait()

        @pl.when(k > 0)
        def _():
            before = k - 1
            wait_fourth(1 - before // chunks, before % chunks)

        slot = k % 2
        total = O2[...]
        for j in range(3):
            total = total + R3[slot, j].astype(F32)
        total = total.astype(BF16)
        B4[...] = total
        OGU[l, :, pl.ds(pl.multiple_of(z * 16, 16), 16), columns(c)] = total[0:2]
        p = S * c + s

        @pl.when(p // chunks == s)
        def _():
            rows, cols = place_d(p, z)
            OD[l, rows, cols] = total[2]

        for copy in spread_gu(l, c):
            copy.start()
        each_d(c, lambda zz: spread_d(l, c, zz).start())

    def layer(li, _):
        l = 1 - li

        def chunk(c, _):
            k = li * chunks + c
            cs = columns(c)

            @pl.when(li == 0)
            def _():
                arrived(1, GU, c)

            @pl.when(li == 0)
            def _():
                for t in range(tiles):
                    r = pl.ds(t * tile, tile)
                    a = A[r, :]
                    g, u = dot(a, WG[1, :, cs], NN), dot(a, WU[1, :, cs], NN)
                    dz = dot(DH[r, :], WD[1, cs, :], NT).astype(BF16).astype(F32)
                    gate = 1.0 / (1.0 + jnp.exp(-g))
                    act = g * gate
                    Z[r, :] = (act * u).astype(BF16)
                    DU[r, cs] = (dz * act).astype(BF16)
                    DG[r, cs] = (dz * (u * (gate + act * (1.0 - gate)))).astype(BF16)

            @pl.when(li == 1)
            def _():
                for t in range(tiles):
                    factors_in(c, t).wait()
                for t in range(tiles):
                    r = pl.ds(t * tile, tile)
                    dz = dot(DH[r, :], WD[0, cs, :], NT).astype(BF16).astype(F32)
                    DU[r, cs] = (dz * F[0, r]).astype(BF16)
                    DG[r, cs] = (dz * F[1, r]).astype(BF16)
                hidden_in(c).wait()

                @pl.when(c < chunks - 1)
                def _():
                    for t in range(tiles):
                        factors_in(c + 1, t).start()

            @pl.when(jnp.logical_and(li == 0, c < chunks - 1))
            def _():
                forward(1, GU, c + 1)

            for back, stage in ((3, stage_3), (2, stage_2), (1, stage_1)):
                @pl.when(c >= back)
                def _(back=back, stage=stage):
                    stage(l, c - back, k - back)

            by_gate = dot(AT[...], DG[:, cs], NN).astype(BF16)
            by_up = dot(AT[...], DU[:, cs], NN).astype(BF16)
            by_down = dot(Z[...], DH[...], ((0,), (0,))).astype(BF16)
            for dev in range(S):
                for q in range(R):
                    to_block = C.at[dev % 2, dev // 2, q]
                    top = rows_d * dev + 16 * q
                    to_block[0] = by_gate[top:top + 16]
                    to_block[1] = by_up[top:top + 16]
                    top = 32 * dev + 16 * (q // 2)
                    to_block[2] = by_down[top:top + 16, (q % 2) * W:(q % 2) * W + W]
            first_hop(k).start()

            @pl.when(jnp.logical_and(li == 1, c < chunks - 1))
            def _():
                hidden_in(c + 1).start()

            return 0

        lax.fori_loop(0, chunks, chunk, 0)

        @pl.when(li == 0)
        def _():
            pltpu.make_async_copy(keep_a, A, keep_sem.at[0]).start()
            pltpu.make_async_copy(keep_at, AT, keep_sem.at[1]).start()
            hidden_in(0).start()
            for t in range(tiles):
                factors_in(0, t).start()

        def below(i, _):
            r = pl.ds(pl.multiple_of(i * small, small), small)
            for q in range(2):
                r2 = pl.ds(pl.multiple_of(i * small + q * fine, fine), fine)
                da = (dot(DG[r2, :], WG[l], NT).astype(BF16).astype(F32)
                      + dot(DU[r2, :], WU[l], NT).astype(BF16).astype(F32)).astype(BF16).astype(F32)
                wide = H[r2, :].astype(F32)
                scale = lax.rsqrt(mean_square(wide))
                along = jnp.mean(da * wide, axis=-1, keepdims=True)
                by_h = (scale * da - wide * (scale * scale * scale * along)).astype(BF16)
                DH[r2, :] = (by_h.astype(F32) + DH[r2, :].astype(F32)).astype(BF16)

            @pl.when(li == 0)
            def _():
                pltpu.make_async_copy(x_ref.at[0, r], H.at[r], in_sem.at[0, i]).start()

            @pl.when(li == 1)
            def _():
                pltpu.make_async_copy(DH.at[r], dx_ref.at[0, r], dx_sem.at[i]).start()

            k = li * chunks + chunks - 1
            for step, stage, back in ((0, stage_3, 2), (0, stage_2, 1), (0, stage_1, 0), (3, stage_3, 1), (3, stage_2, 0), (5, stage_3, 0)):
                @pl.when(i == step * few // 8)
                def _(stage=stage, back=back):
                    stage(l, chunks - 1 - back, k - back)

            return 0

        lax.fori_loop(0, few, below, 0)

        @pl.when(li == 0)
        def _():
            pltpu.make_async_copy(keep_a, A, keep_sem.at[0]).wait()
            pltpu.make_async_copy(keep_at, AT, keep_sem.at[1]).wait()
            for i in range(few):
                x_in(i)[0].wait()

        return 0

    lax.fori_loop(0, 2, layer, 0)

    wait_fourth(0, chunks - 1)
    for l in range(2):
        for c in range(chunks):
            for copy in spread_gu(l, c):
                copy.wait_recv()
        for pos in range(chunks):
            p = s * chunks + pos
            for zz in range(R):
                @pl.when(jnp.logical_not(jnp.logical_and(p % S == s, z == zz)))
                def _(l=l, pos=pos, zz=zz):
                    rows, cols = place_d(pos, zz)
                    to(s4_sem.at[0], rd_sem.at[l, pos, zz], B4.at[2], OD.at[l, rows, cols], z, s).wait_recv()
    last = (pltpu.make_async_copy(OGU.at[:, 0], og_ref, out_sem.at[0]),
            pltpu.make_async_copy(OGU.at[:, 1], ou_ref, out_sem.at[1]),
            pltpu.make_async_copy(OD, od_ref, out_sem.at[2]))
    for copy in last:
        copy.start()
    for l in range(2):
        sent(l, DOWN, 0)

        def all_sent(c, _, l=l):
            sent(l, GU, c)
            return 0

        lax.fori_loop(0, chunks, all_sent, 0)
    for i in range(few):
        r = pl.ds(i * small, small)
        pltpu.make_async_copy(DH.at[r], dx_ref.at[0, r], dx_sem.at[i]).wait()
    for copy in last:
        copy.wait()


def whole(tokens, d, ff):
    tile, small = min(1024, tokens // 4), min(512, tokens // 8)
    few = tokens // small
    chunks = ff // W
    dma = pltpu.SemaphoreType.DMA
    layers = 2
    shape = jax.ShapeDtypeStruct
    rows_d, rows_f = d // S, ff // S
    any_space = pl.BlockSpec(memory_space=pl.ANY)
    flops = 2 * tokens * d * ff * 17
    return pl.pallas_call(
        functools.partial(kernel, tokens, d, ff, tile, small),
        out_shape=(
            shape((1, tokens, d), BF16), shape((layers, rows_d, ff), BF16), shape((layers, rows_d, ff), BF16),
            shape((layers, rows_f, d), BF16), shape((tokens, d), BF16), shape((d, tokens), BF16),
            shape((chunks, 2, tokens, W), F32), shape((tokens, ff), BF16)),
        in_specs=[any_space] * 5,
        out_specs=(any_space,) * 8,
        scratch_shapes=[
            pltpu.VMEM((layers, d, ff), BF16), pltpu.VMEM((layers, d, ff), BF16), pltpu.VMEM((layers, ff, d), BF16),
            pltpu.VMEM((tokens, d), BF16), pltpu.VMEM((d, tokens), BF16),
            pltpu.VMEM((tokens, d), BF16), pltpu.VMEM((tokens, d), BF16),
            pltpu.VMEM((tokens, ff), BF16), pltpu.VMEM((tokens, ff), BF16),
            pltpu.VMEM((tokens, W), BF16), pltpu.VMEM((2, tokens, W), F32),
            pltpu.VMEM((2, 4, R, 3, 16, W), BF16), pltpu.VMEM((2, 4, R, 3, 16, W), BF16),
            pltpu.VMEM((R, 3, 16, W), F32), pltpu.VMEM((4, R, 3, 16, W), BF16),
            pltpu.VMEM((2, 3, R, 3, 16, W), BF16), pltpu.VMEM((3, 16, W), F32),
            pltpu.VMEM((R, 3, 16, W), BF16), pltpu.VMEM((2, 3, 3, 16, W), BF16),
            pltpu.VMEM((3, 16, W), BF16),
            pltpu.VMEM((layers, 2, rows_d, ff), BF16), pltpu.VMEM((layers, rows_f, d), BF16),
            dma((2, few)), dma((layers, 3)), dma((2,)),
            dma((layers, 3, chunks, 4)), dma((layers, 3, chunks, 4)), dma((layers, 3, chunks, 3)), dma((layers, 3, chunks, 3)),
            dma((1,)), dma((2,)), dma((3,)), dma((2, 3)), dma((3,)), dma((2, 3)),
            dma((7,)), dma((layers, chunks, 3)), dma((layers, chunks, R)), dma((3,)), dma((few,)), dma((tokens // tile,)), dma((1,)),
        ],
        compiler_params=pltpu.CompilerParams(has_side_effects=True, collective_id=0, vmem_limit_bytes=67_043_328),
        cost_estimate=pl.CostEstimate(flops=flops, bytes_accessed=4 * tokens * d * 2, transcendentals=0),
        name="stack",
    )


def solution(mesh):
    def step(x, dy, w_gate, w_up, w_down):
        _, tokens, d = x.shape
        ff = w_gate.shape[2]
        return whole(tokens, d, ff)(x, dy, w_gate, w_up, w_down)[:4]

    states, cut = P(("rep", "r", "s"), None, None), P(None, "s", None)
    return jax.shard_map(
        step,
        mesh=mesh,
        in_specs=(states, states) + (cut,) * 3,
        out_specs=(states,) + (P("rep", "s", None),) * 3,
        check_vma=False,
    )
```

```python
import functools

import jax
import jax.numpy as jnp
from jax import lax
from jax.experimental import pallas as pl
from jax.experimental.pallas import tpu as pltpu
from jax.sharding import PartitionSpec as P

MESH = pl.DeviceIdType.MESH
F32, BF16 = jnp.float32, jnp.bfloat16
W = 256
S, R = 8, 4


def dot(a, b, dims):
    return lax.dot_general(a, b, (dims, ((), ())), preferred_element_type=F32)


NN, NT = ((1,), (0,)), ((1,), (1,))


def mean_square(wide):
    return jnp.mean(wide * wide, axis=-1, keepdims=True) + 1e-6


def kernel(
    tokens, d, ff, tile, small,
    x_ref, dy_ref, wg_ref, wu_ref, wd_ref,
    dx_ref, og_ref, ou_ref, od_ref, keep_a, keep_at, keep_f, keep_z,
    WG, WU, WD, A, AT, H, DH, DG, DU, Z, F,
    C, R1, O1, B2, R2, O2, B3, R3, B4, OGU, OD,
    in_sem, own_sem, keep_sem, gs_sem, gr_sem, fs_sem, fr_sem,
    s1_sem, r1_sem, s2_sem, r2_sem, s3_sem, r3_sem, s4_sem, r4_sem, rd_sem, out_sem, dx_sem, f_sem, z_sem,
):
    z, s = lax.axis_index("r"), lax.axis_index("s")
    core, yy, xx = s % 2, (s // 2) % 2, s // 4
    xy = s // 2
    chunks = ff // W
    rows_d, rows_f = d // S, ff // S

    def at(px, py, pc):
        return 4 * px + 2 * py + pc

    def to(sem_s, sem_r, src, dst, r, dev):
        return pltpu.make_async_remote_copy(
            src_ref=src, dst_ref=dst, send_sem=sem_s, recv_sem=sem_r,
            device_id={"r": r, "s": dev}, device_id_type=MESH)

    sib = at(xx, yy, 1 - core)
    others = (at(1 - xx, yy, core), at(xx, 1 - yy, core), at(1 - xx, 1 - yy, core))

    mats = ((wg_ref, WG, rows_d), (wu_ref, WU, rows_d), (wd_ref, WD, rows_f))

    def columns(c):
        return pl.ds(pl.multiple_of(c * W, W), W)

    def piece(l, m, c, dev):
        _, full, rows = mats[m]
        r = pl.ds(pl.multiple_of(dev * rows, rows), rows)
        return full.at[l, r] if m == 2 else full.at[l, r, columns(c)]

    def mine(l, m, c):
        return mats[m][0].at[l] if m == 2 else mats[m][0].at[l, :, columns(c)]

    def spread(l, m, c, i):
        return to(gs_sem.at[l, m, c, i], gr_sem.at[l, m, c, i], mine(l, m, c), piece(l, m, c, s), z, (others + (sib,))[i])

    def onward(l, m, c, i):
        block = piece(l, m, c, others[i])
        return to(fs_sem.at[l, m, c, i], fr_sem.at[l, m, c, i], block, block, z, sib)

    def own(l, m):
        rows = mats[m][2]
        return pltpu.make_async_copy(
            mats[m][0].at[l], mats[m][1].at[l, pl.ds(pl.multiple_of(s * rows, rows), rows)], own_sem.at[l, m])

    def send(l, ms, c):
        for m in ms:
            for i in range(4):
                spread(l, m, c, i).start()

    def forward(l, ms, c):
        for m in ms:
            for i in range(3):
                spread(l, m, c, i).wait_recv()
                onward(l, m, c, i).start()

    def arrived(l, ms, c):
        for m in ms:
            spread(l, m, c, 3).wait_recv()
            for i in range(3):
                onward(l, m, c, i).wait_recv()

    def sent(l, ms, c):
        for m in ms:
            for i in range(4):
                spread(l, m, c, i).wait_send()
            for i in range(3):
                onward(l, m, c, i).wait_send()

    GU, DOWN = (0, 1), (2,)
    barrier = pltpu.get_barrier_semaphore()
    here = z * S + s

    def greet(i, _):
        there = (here + i) % (R * S)
        pl.semaphore_signal(barrier, inc=1, device_id={"r": there // S, "s": there % S}, device_id_type=MESH)
        return 0

    lax.fori_loop(1, R * S, greet, 0)
    tiles, few = tokens // tile, tokens // small
    fine = small // 2
    down_parts = tokens // fine

    def x_in(i):
        r = pl.ds(i * small, small)
        return (pltpu.make_async_copy(x_ref.at[0, r], H.at[r], in_sem.at[0, i]),
                pltpu.make_async_copy(dy_ref.at[0, r], DH.at[r], in_sem.at[1, i]))

    for i in range(few):
        for copy in x_in(i):
            copy.start()
    for l in range(2):
        for m in range(3):
            own(l, m).start()

    def enter(i, _):
        r = pl.ds(pl.multiple_of(i * small, small), small)
        pltpu.make_async_copy(x_ref.at[0, r], H.at[r], in_sem.at[0, i]).wait()
        wide = H[r, :].astype(F32)
        a = (wide * lax.rsqrt(mean_square(wide))).astype(BF16)
        A[r, :] = a
        AT[:, r] = a.T
        return 0

    lax.fori_loop(0, few, enter, 0)
    pl.semaphore_wait(barrier, R * S - 1)
    for c in range(chunks):
        send(0, GU, c)
    send(0, DOWN, 0)
    keep = (pltpu.make_async_copy(A, keep_a, keep_sem.at[0]), pltpu.make_async_copy(AT, keep_at, keep_sem.at[1]))
    for copy in keep:
        copy.start()

    forward(0, GU, 0)
    send(1, DOWN, 0)
    for c in range(chunks):
        send(1, GU, c)
    for l in range(2):
        for m in range(3):
            own(l, m).wait()

    def factors_out(c, t):
        r = pl.ds(pl.multiple_of(t * tile, tile), tile)
        return pltpu.make_async_copy(F.at[:, r], keep_f.at[c, :, r], f_sem.at[t])

    def factors_in(c, t):
        r = pl.ds(t * tile, tile)
        return pltpu.make_async_copy(keep_f.at[c, :, r], F.at[:, r], f_sem.at[t])

    def hidden_in(c):
        return pltpu.make_async_copy(keep_z.at[:, columns(c)], Z, z_sem.at[0])

    def gated(i, _):
        c, t = i // tiles, i % tiles
        r, cs = pl.ds(pl.multiple_of(t * tile, tile), tile), columns(c)

        @pl.when(t == 0)
        def _():
            arrived(0, GU, c)

        @pl.when(c > 0)
        def _():
            factors_out(c - 1, t).wait()

        a = A[r, :]
        g, u = dot(a, WG[0, :, cs], NN), dot(a, WU[0, :, cs], NN)
        gate = 1.0 / (1.0 + jnp.exp(-g))
        act = g * gate
        DG[r, cs] = (act * u).astype(BF16)
        F[0, r] = act
        F[1, r] = u * (gate + act * (1.0 - gate))
        factors_out(c, t).start()

        @pl.when(jnp.logical_and(t == 2, c < chunks - 1))
        def _():
            forward(0, GU, c + 1)

        return 0

    lax.fori_loop(0, chunks * tiles, gated, 0)
    all_hidden = pltpu.make_async_copy(DG, keep_z, z_sem.at[0])
    all_hidden.start()
    forward(0, DOWN, 0)
    for i in range(few):
        x_in(i)[1].wait()
    arrived(0, DOWN, 0)
    for copy in keep:
        copy.wait()

    def down(i, _):
        for q in range(down_parts // 2):
            r = pl.ds(pl.multiple_of((i * (down_parts // 2) + q) * fine, fine), fine)
            h = (H[r, :].astype(F32) + dot(DG[r, :], WD[0], NN).astype(BF16).astype(F32)).astype(BF16)
            H[r, :] = h
            wide = h.astype(F32)
            a = (wide * lax.rsqrt(mean_square(wide))).astype(BF16)
            A[r, :] = a
            AT[:, r] = a.T

        @pl.when(i == 0)
        def _():
            forward(1, DOWN, 0)

        return 0

    lax.fori_loop(0, 2, down, 0)
    forward(1, GU, 0)
    arrived(1, DOWN, 0)
    all_hidden.wait()
    for t in range(tiles):
        factors_out(chunks - 1, t).wait()

    def first_hop(k):
        slot = k % 2
        return to(s1_sem.at[0], r1_sem.at[slot], C.at[1 - core], R1.at[slot], z, sib)

    def second_hop(k):
        slot = k % 2
        places = ((1 - xx) * 2 + yy, xx * 2 + 1 - yy, (1 - xx) * 2 + 1 - yy)
        return [to(s2_sem.at[i], r2_sem.at[slot, i], B2.at[places[i]], R2.at[slot, i], z, others[i]) for i in range(3)]

    def third_hop(k):
        slot = k % 2
        return [to(s3_sem.at[i], r3_sem.at[slot, i], B3.at[(z + 1 + i) % R], R3.at[slot, i], (z + 1 + i) % R, s)
                for i in range(3)]

    def spread_gu(l, c):
        return [to(s4_sem.at[i], r4_sem.at[l, c, i], B4.at[pl.ds(0, 2)],
                   OGU.at[l, :, pl.ds(pl.multiple_of(z * 16, 16), 16), columns(c)], (z + 1 + i) % R, s)
                for i in range(3)]

    def place_d(p, zz):
        return (pl.ds(pl.multiple_of((p % chunks) * 32 + (zz // 2) * 16, 16), 16),
                pl.ds(pl.multiple_of((zz % 2) * W, W), W))

    def spread_d(l, c, zz):
        p = S * c + s
        rows, cols = place_d(p, z)
        return to(s4_sem.at[3 + zz], rd_sem.at[l, p % chunks, z], B4.at[2], OD.at[l, rows, cols], zz, p // chunks)

    def each_d(c, fn):
        for zz in range(R):
            @pl.when(jnp.logical_not(jnp.logical_and((S * c + s) // chunks == s, z == zz)))
            def _(zz=zz):
                fn(zz)

    def wait_fourth(l, c):
        for copy in spread_gu(l, c):
            copy.wait_send()
        each_d(c, lambda zz: spread_d(l, c, zz).wait_send())

    def stage_1(l, c, k):
        first_hop(k).wait()
        slot = k % 2
        B2[...] = (C[core].astype(F32) + R1[slot].astype(F32)).astype(BF16)
        O1[...] = C[core, xy].astype(F32) + R1[slot, xy].astype(F32)
        for copy in second_hop(k):
            copy.start()

    def stage_2(l, c, k):
        for copy in second_hop(k):
            copy.wait()
        slot = k % 2
        B3[...] = (O1[...] + R2[slot, 0].astype(F32) + R2[slot, 1].astype(F32) + R2[slot, 2].astype(F32)).astype(BF16)
        O2[...] = O1[z] + R2[slot, 0, z].astype(F32) + R2[slot, 1, z].astype(F32) + R2[slot, 2, z].astype(F32)
        for copy in third_hop(k):
            copy.start()

    def stage_3(l, c, k):
        for copy in third_hop(k):
            copy.wait()

        @pl.when(k > 0)
        def _():
            before = k - 1
            wait_fourth(1 - before // chunks, before % chunks)

        slot = k % 2
        total = O2[...]
        for j in range(3):
            total = total + R3[slot, j].astype(F32)
        total = total.astype(BF16)
        B4[...] = total
        OGU[l, :, pl.ds(pl.multiple_of(z * 16, 16), 16), columns(c)] = total[0:2]
        p = S * c + s

        @pl.when(p // chunks == s)
        def _():
            rows, cols = place_d(p, z)
            OD[l, rows, cols] = total[2]

        for copy in spread_gu(l, c):
            copy.start()
        each_d(c, lambda zz: spread_d(l, c, zz).start())

    def layer(li, _):
        l = 1 - li

        def chunk(c, _):
            k = li * chunks + c
            cs = columns(c)

            @pl.when(li == 0)
            def _():
                arrived(1, GU, c)

            @pl.when(li == 0)
            def _():
                for t in range(tiles):
                    r = pl.ds(t * tile, tile)
                    a = A[r, :]
                    g, u = dot(a, WG[1, :, cs], NN), dot(a, WU[1, :, cs], NN)
                    dz = dot(DH[r, :], WD[1, cs, :], NT).astype(BF16).astype(F32)
                    gate = 1.0 / (1.0 + jnp.exp(-g))
                    act = g * gate
                    Z[r, :] = (act * u).astype(BF16)
                    DU[r, cs] = (dz * act).astype(BF16)
                    DG[r, cs] = (dz * (u * (gate + act * (1.0 - gate)))).astype(BF16)

            @pl.when(li == 1)
            def _():
                for t in range(tiles):
                    factors_in(c, t).wait()
                for t in range(tiles):
                    r = pl.ds(t * tile, tile)
                    dz = dot(DH[r, :], WD[0, cs, :], NT).astype(BF16).astype(F32)
                    DU[r, cs] = (dz * F[0, r]).astype(BF16)
                    DG[r, cs] = (dz * F[1, r]).astype(BF16)
                hidden_in(c).wait()

                @pl.when(c < chunks - 1)
                def _():
                    for t in range(tiles):
                        factors_in(c + 1, t).start()

            @pl.when(jnp.logical_and(li == 0, c < chunks - 1))
            def _():
                forward(1, GU, c + 1)

            for back, stage in ((3, stage_3), (2, stage_2), (1, stage_1)):
                @pl.when(c >= back)
                def _(back=back, stage=stage):
                    stage(l, c - back, k - back)

            by_gate = dot(AT[...], DG[:, cs], NN).astype(BF16)
            by_up = dot(AT[...], DU[:, cs], NN).astype(BF16)
            by_down = dot(Z[...], DH[...], ((0,), (0,))).astype(BF16)
            for dev in range(S):
                for q in range(R):
                    to_block = C.at[dev % 2, dev // 2, q]
                    top = rows_d * dev + 16 * q
                    to_block[0] = by_gate[top:top + 16]
                    to_block[1] = by_up[top:top + 16]
                    top = 32 * dev + 16 * (q // 2)
                    to_block[2] = by_down[top:top + 16, (q % 2) * W:(q % 2) * W + W]
            first_hop(k).start()

            @pl.when(jnp.logical_and(li == 1, c < chunks - 1))
            def _():
                hidden_in(c + 1).start()

            return 0

        lax.fori_loop(0, chunks, chunk, 0)

        @pl.when(li == 0)
        def _():
            pltpu.make_async_copy(keep_a, A, keep_sem.at[0]).start()
            pltpu.make_async_copy(keep_at, AT, keep_sem.at[1]).start()
            hidden_in(0).start()
            for t in range(tiles):
                factors_in(0, t).start()

        def below(i, _):
            r = pl.ds(pl.multiple_of(i * small, small), small)
            for q in range(2):
                r2 = pl.ds(pl.multiple_of(i * small + q * fine, fine), fine)
                da = (dot(DG[r2, :], WG[l], NT).astype(BF16).astype(F32)
                      + dot(DU[r2, :], WU[l], NT).astype(BF16).astype(F32)).astype(BF16).astype(F32)
                wide = H[r2, :].astype(F32)
                scale = lax.rsqrt(mean_square(wide))
                along = jnp.mean(da * wide, axis=-1, keepdims=True)
                by_h = (scale * da - wide * (scale * scale * scale * along)).astype(BF16)
                DH[r2, :] = (by_h.astype(F32) + DH[r2, :].astype(F32)).astype(BF16)

            @pl.when(li == 0)
            def _():
                pltpu.make_async_copy(x_ref.at[0, r], H.at[r], in_sem.at[0, i]).start()

            @pl.when(li == 1)
            def _():
                pltpu.make_async_copy(DH.at[r], dx_ref.at[0, r], dx_sem.at[i]).start()

            k = li * chunks + chunks - 1
            for step, stage, back in ((0, stage_3, 2), (0, stage_2, 1), (0, stage_1, 0), (3, stage_3, 1), (3, stage_2, 0), (5, stage_3, 0)):
                @pl.when(i == step * few // 8)
                def _(stage=stage, back=back):
                    stage(l, chunks - 1 - back, k - back)

            return 0

        lax.fori_loop(0, few, below, 0)

        @pl.when(li == 0)
        def _():
            pltpu.make_async_copy(keep_a, A, keep_sem.at[0]).wait()
            pltpu.make_async_copy(keep_at, AT, keep_sem.at[1]).wait()
            for i in range(few):
                x_in(i)[0].wait()

        return 0

    lax.fori_loop(0, 2, layer, 0)

    wait_fourth(0, chunks - 1)
    for l in range(2):
        for c in range(chunks):
            for copy in spread_gu(l, c):
                copy.wait_recv()
        for pos in range(chunks):
            p = s * chunks + pos
            for zz in range(R):
                @pl.when(jnp.logical_not(jnp.logical_and(p % S == s, z == zz)))
                def _(l=l, pos=pos, zz=zz):
                    rows, cols = place_d(pos, zz)
                    to(s4_sem.at[0], rd_sem.at[l, pos, zz], B4.at[2], OD.at[l, rows, cols], z, s).wait_recv()
    last = (pltpu.make_async_copy(OGU.at[:, 0], og_ref, out_sem.at[0]),
            pltpu.make_async_copy(OGU.at[:, 1], ou_ref, out_sem.at[1]),
            pltpu.make_async_copy(OD, od_ref, out_sem.at[2]))
    for copy in last:
        copy.start()
    for l in range(2):
        sent(l, DOWN, 0)

        def all_sent(c, _, l=l):
            sent(l, GU, c)
            return 0

        lax.fori_loop(0, chunks, all_sent, 0)
    for i in range(few):
        r = pl.ds(i * small, small)
        pltpu.make_async_copy(DH.at[r], dx_ref.at[0, r], dx_sem.at[i]).wait()
    for copy in last:
        copy.wait()


def whole(tokens, d, ff):
    tile, small = min(1024, tokens // 4), min(512, tokens // 8)
    few = tokens // small
    chunks = ff // W
    dma = pltpu.SemaphoreType.DMA
    layers = 2
    shape = jax.ShapeDtypeStruct
    rows_d, rows_f = d // S, ff // S
    any_space = pl.BlockSpec(memory_space=pl.ANY)
    flops = 2 * tokens * d * ff * 17
    return pl.pallas_call(
        functools.partial(kernel, tokens, d, ff, tile, small),
        out_shape=(
            shape((1, tokens, d), BF16), shape((layers, rows_d, ff), BF16), shape((layers, rows_d, ff), BF16),
            shape((layers, rows_f, d), BF16), shape((tokens, d), BF16), shape((d, tokens), BF16),
            shape((chunks, 2, tokens, W), F32), shape((tokens, ff), BF16)),
        in_specs=[any_space] * 5,
        out_specs=(any_space,) * 8,
        scratch_shapes=[
            pltpu.VMEM((layers, d, ff), BF16), pltpu.VMEM((layers, d, ff), BF16), pltpu.VMEM((layers, ff, d), BF16),
            pltpu.VMEM((tokens, d), BF16), pltpu.VMEM((d, tokens), BF16),
            pltpu.VMEM((tokens, d), BF16), pltpu.VMEM((tokens, d), BF16),
            pltpu.VMEM((tokens, ff), BF16), pltpu.VMEM((tokens, ff), BF16),
            pltpu.VMEM((tokens, W), BF16), pltpu.VMEM((2, tokens, W), F32),
            pltpu.VMEM((2, 4, R, 3, 16, W), BF16), pltpu.VMEM((2, 4, R, 3, 16, W), BF16),
            pltpu.VMEM((R, 3, 16, W), F32), pltpu.VMEM((4, R, 3, 16, W), BF16),
            pltpu.VMEM((2, 3, R, 3, 16, W), BF16), pltpu.VMEM((3, 16, W), F32),
            pltpu.VMEM((R, 3, 16, W), BF16), pltpu.VMEM((2, 3, 3, 16, W), BF16),
            pltpu.VMEM((3, 16, W), BF16),
            pltpu.VMEM((layers, 2, rows_d, ff), BF16), pltpu.VMEM((layers, rows_f, d), BF16),
            dma((2, few)), dma((layers, 3)), dma((2,)),
            dma((layers, 3, chunks, 4)), dma((layers, 3, chunks, 4)), dma((layers, 3, chunks, 3)), dma((layers, 3, chunks, 3)),
            dma((1,)), dma((2,)), dma((3,)), dma((2, 3)), dma((3,)), dma((2, 3)),
            dma((7,)), dma((layers, chunks, 3)), dma((layers, chunks, R)), dma((3,)), dma((few,)), dma((tokens // tile,)), dma((1,)),
        ],
        compiler_params=pltpu.CompilerParams(has_side_effects=True, collective_id=0, vmem_limit_bytes=67_043_328),
        cost_estimate=pl.CostEstimate(flops=flops, bytes_accessed=4 * tokens * d * 2, transcendentals=0),
        name="stack",
    )


def hand_on(*refs):
    n = len(refs) // 4
    ins, outs, held, (sems,) = refs[:4], refs[4:8], refs[8:12], refs[12:]
    parts = [(0, slice(512 * i, 512 * (i + 1))) for i in range(ins[0].shape[1] // 512)]
    jobs = [(0, part) for part in parts] + [(i, (slice(None),)) for i in range(1, n + 3) if i < 4]
    copies = []
    for q, (i, (*lead, rows)) in enumerate(jobs):
        at = (*lead, pl.ds(rows.start, 512)) if rows.start is not None else (pl.ds(0, ins[i].shape[0]),)
        copies.append((pltpu.make_async_copy(ins[i].at[at], held[i].at[at], sems.at[0, q]),
                       pltpu.make_async_copy(held[i].at[at], outs[i].at[at], sems.at[1, q])))
    for into, _ in copies:
        into.start()
    for into, out in copies:
        into.wait()
        out.start()
    for _, out in copies:
        out.wait()


def handed_on(*arrays):
    any_space = pl.BlockSpec(memory_space=pl.ANY)
    jobs = arrays[0].shape[1] // 512 + 3
    return pl.pallas_call(
        hand_on,
        out_shape=tuple(jax.ShapeDtypeStruct(a.shape, a.dtype) for a in arrays),
        in_specs=[any_space] * 4,
        out_specs=(any_space,) * 4,
        scratch_shapes=[pltpu.VMEM(a.shape, a.dtype) for a in arrays] + [pltpu.SemaphoreType.DMA((2, jobs))],
        name="hand_on",
    )(*arrays)


def solution(mesh):
    def step(x, dy, w_gate, w_up, w_down):
        _, tokens, d = x.shape
        ff = w_gate.shape[2]
        return handed_on(*whole(tokens, d, ff)(x, dy, w_gate, w_up, w_down)[:4])

    states, cut = P(("rep", "r", "s"), None, None), P(None, "s", None)
    return jax.shard_map(
        step,
        mesh=mesh,
        in_specs=(states, states) + (cut,) * 3,
        out_specs=(states,) + (P("rep", "s", None),) * 3,
        check_vma=False,
    )
```

```python
import functools

import jax
import jax.numpy as jnp
from jax import lax
from jax.experimental import pallas as pl
from jax.experimental.pallas import tpu as pltpu
from jax.sharding import PartitionSpec as P

MESH = pl.DeviceIdType.MESH
F32, BF16 = jnp.float32, jnp.bfloat16
W = 256
S, R = 8, 4


def dot(a, b, dims):
    return lax.dot_general(a, b, (dims, ((), ())), preferred_element_type=F32)


NN, NT = ((1,), (0,)), ((1,), (1,))


def mean_square(wide):
    return jnp.mean(wide * wide, axis=-1, keepdims=True) + 1e-6


def kernel(
    tokens, d, ff, tile, small,
    x_ref, dy_ref, wg_ref, wu_ref, wd_ref,
    dx_ref, og_ref, ou_ref, od_ref, keep_a, keep_at, keep_f, keep_z,
    WG, WU, WD, A, AT, H, DH, DG, DU, Z, F,
    C, R1, O1, B2, R2, O2, B3, R3, B4, OGU, OD,
    in_sem, own_sem, keep_sem, gs_sem, gr_sem, fs_sem, fr_sem,
    s1_sem, r1_sem, s2_sem, r2_sem, s3_sem, r3_sem, s4_sem, r4_sem, rd_sem, out_sem, dx_sem, f_sem, z_sem,
):
    z, s = lax.axis_index("r"), lax.axis_index("s")
    core, yy, xx = s % 2, (s // 2) % 2, s // 4
    xy = s // 2
    chunks = ff // W
    rows_d, rows_f = d // S, ff // S

    def at(px, py, pc):
        return 4 * px + 2 * py + pc

    def to(sem_s, sem_r, src, dst, r, dev):
        return pltpu.make_async_remote_copy(
            src_ref=src, dst_ref=dst, send_sem=sem_s, recv_sem=sem_r,
            device_id={"r": r, "s": dev}, device_id_type=MESH)

    sib = at(xx, yy, 1 - core)
    others = (at(1 - xx, yy, core), at(xx, 1 - yy, core), at(1 - xx, 1 - yy, core))

    mats = ((wg_ref, WG, rows_d), (wu_ref, WU, rows_d), (wd_ref, WD, rows_f))

    def columns(c):
        return pl.ds(pl.multiple_of(c * W, W), W)

    def piece(l, m, c, dev):
        _, full, rows = mats[m]
        r = pl.ds(pl.multiple_of(dev * rows, rows), rows)
        return full.at[l, r] if m == 2 else full.at[l, r, columns(c)]

    def mine(l, m, c):
        return mats[m][0].at[l] if m == 2 else mats[m][0].at[l, :, columns(c)]

    def spread(l, m, c, i):
        return to(gs_sem.at[l, m, c, i], gr_sem.at[l, m, c, i], mine(l, m, c), piece(l, m, c, s), z, (others + (sib,))[i])

    def onward(l, m, c, i):
        block = piece(l, m, c, others[i])
        return to(fs_sem.at[l, m, c, i], fr_sem.at[l, m, c, i], block, block, z, sib)

    def own(l, m):
        rows = mats[m][2]
        return pltpu.make_async_copy(
            mats[m][0].at[l], mats[m][1].at[l, pl.ds(pl.multiple_of(s * rows, rows), rows)], own_sem.at[l, m])

    def send(l, ms, c):
        for m in ms:
            for i in range(4):
                spread(l, m, c, i).start()

    def forward(l, ms, c):
        for m in ms:
            for i in range(3):
                spread(l, m, c, i).wait_recv()
                onward(l, m, c, i).start()

    def arrived(l, ms, c):
        for m in ms:
            spread(l, m, c, 3).wait_recv()
            for i in range(3):
                onward(l, m, c, i).wait_recv()

    def sent(l, ms, c):
        for m in ms:
            for i in range(4):
                spread(l, m, c, i).wait_send()
            for i in range(3):
                onward(l, m, c, i).wait_send()

    GU, DOWN = (0, 1), (2,)
    barrier = pltpu.get_barrier_semaphore()
    here = z * S + s

    def greet(i, _):
        there = (here + i) % (R * S)
        pl.semaphore_signal(barrier, inc=1, device_id={"r": there // S, "s": there % S}, device_id_type=MESH)
        return 0

    lax.fori_loop(1, R * S, greet, 0)
    tiles, few = tokens // tile, tokens // small
    fine = small // 2
    down_parts = tokens // fine

    def x_in(i):
        r = pl.ds(i * small, small)
        return (pltpu.make_async_copy(x_ref.at[0, r], H.at[r], in_sem.at[0, i]),
                pltpu.make_async_copy(dy_ref.at[0, r], DH.at[r], in_sem.at[1, i]))

    for i in range(few):
        for copy in x_in(i):
            copy.start()
    for l in range(2):
        for m in range(3):
            own(l, m).start()

    def enter(i, _):
        r = pl.ds(pl.multiple_of(i * small, small), small)
        pltpu.make_async_copy(x_ref.at[0, r], H.at[r], in_sem.at[0, i]).wait()
        wide = H[r, :].astype(F32)
        a = (wide * lax.rsqrt(mean_square(wide))).astype(BF16)
        A[r, :] = a
        AT[:, r] = a.T
        return 0

    lax.fori_loop(0, few, enter, 0)
    pl.semaphore_wait(barrier, R * S - 1)
    for c in range(chunks):
        send(0, GU, c)
    send(0, DOWN, 0)
    keep = (pltpu.make_async_copy(A, keep_a, keep_sem.at[0]), pltpu.make_async_copy(AT, keep_at, keep_sem.at[1]))
    for copy in keep:
        copy.start()

    forward(0, GU, 0)
    send(1, DOWN, 0)
    for c in range(chunks):
        send(1, GU, c)
    for l in range(2):
        for m in range(3):
            own(l, m).wait()

    def factors_out(c, t):
        r = pl.ds(pl.multiple_of(t * tile, tile), tile)
        return pltpu.make_async_copy(F.at[:, r], keep_f.at[c, :, r], f_sem.at[t])

    def factors_in(c, t):
        r = pl.ds(t * tile, tile)
        return pltpu.make_async_copy(keep_f.at[c, :, r], F.at[:, r], f_sem.at[t])

    def hidden_in(c):
        return pltpu.make_async_copy(keep_z.at[:, columns(c)], Z, z_sem.at[0])

    def gated(i, _):
        c, t = i // tiles, i % tiles
        r, cs = pl.ds(pl.multiple_of(t * tile, tile), tile), columns(c)

        @pl.when(t == 0)
        def _():
            arrived(0, GU, c)

        @pl.when(c > 0)
        def _():
            factors_out(c - 1, t).wait()

        a = A[r, :]
        g, u = dot(a, WG[0, :, cs], NN), dot(a, WU[0, :, cs], NN)
        gate = 1.0 / (1.0 + jnp.exp(-g))
        act = g * gate
        DG[r, cs] = (act * u).astype(BF16)
        F[0, r] = act
        F[1, r] = u * (gate + act * (1.0 - gate))
        factors_out(c, t).start()

        @pl.when(jnp.logical_and(t == 2, c < chunks - 1))
        def _():
            forward(0, GU, c + 1)

        return 0

    lax.fori_loop(0, chunks * tiles, gated, 0)
    all_hidden = pltpu.make_async_copy(DG, keep_z, z_sem.at[0])
    all_hidden.start()
    forward(0, DOWN, 0)
    for i in range(few):
        x_in(i)[1].wait()
    arrived(0, DOWN, 0)
    for copy in keep:
        copy.wait()

    def down(i, _):
        for q in range(down_parts // 2):
            r = pl.ds(pl.multiple_of((i * (down_parts // 2) + q) * fine, fine), fine)
            h = (H[r, :].astype(F32) + dot(DG[r, :], WD[0], NN).astype(BF16).astype(F32)).astype(BF16)
            H[r, :] = h
            wide = h.astype(F32)
            a = (wide * lax.rsqrt(mean_square(wide))).astype(BF16)
            A[r, :] = a
            AT[:, r] = a.T

        @pl.when(i == 0)
        def _():
            forward(1, DOWN, 0)

        return 0

    lax.fori_loop(0, 2, down, 0)
    forward(1, GU, 0)
    arrived(1, DOWN, 0)
    all_hidden.wait()
    for t in range(tiles):
        factors_out(chunks - 1, t).wait()

    def first_hop(k):
        slot = k % 2
        return to(s1_sem.at[0], r1_sem.at[slot], C.at[1 - core], R1.at[slot], z, sib)

    def second_hop(k):
        slot = k % 2
        places = ((1 - xx) * 2 + yy, xx * 2 + 1 - yy, (1 - xx) * 2 + 1 - yy)
        return [to(s2_sem.at[i], r2_sem.at[slot, i], B2.at[places[i]], R2.at[slot, i], z, others[i]) for i in range(3)]

    def third_hop(k):
        slot = k % 2
        return [to(s3_sem.at[i], r3_sem.at[slot, i], B3.at[(z + 1 + i) % R], R3.at[slot, i], (z + 1 + i) % R, s)
                for i in range(3)]

    def spread_gu(l, c):
        return [to(s4_sem.at[i], r4_sem.at[l, c, i], B4.at[pl.ds(0, 2)],
                   OGU.at[l, :, pl.ds(pl.multiple_of(z * 16, 16), 16), columns(c)], (z + 1 + i) % R, s)
                for i in range(3)]

    def place_d(p, zz):
        return (pl.ds(pl.multiple_of((p % chunks) * 32 + (zz // 2) * 16, 16), 16),
                pl.ds(pl.multiple_of((zz % 2) * W, W), W))

    def spread_d(l, c, zz):
        p = S * c + s
        rows, cols = place_d(p, z)
        return to(s4_sem.at[3 + zz], rd_sem.at[l, p % chunks, z], B4.at[2], OD.at[l, rows, cols], zz, p // chunks)

    def each_d(c, fn):
        for zz in range(R):
            @pl.when(jnp.logical_not(jnp.logical_and((S * c + s) // chunks == s, z == zz)))
            def _(zz=zz):
                fn(zz)

    def wait_fourth(l, c):
        for copy in spread_gu(l, c):
            copy.wait_send()
        each_d(c, lambda zz: spread_d(l, c, zz).wait_send())

    def stage_1(l, c, k):
        first_hop(k).wait()
        slot = k % 2
        B2[...] = (C[core].astype(F32) + R1[slot].astype(F32)).astype(BF16)
        O1[...] = C[core, xy].astype(F32) + R1[slot, xy].astype(F32)
        for copy in second_hop(k):
            copy.start()

    def stage_2(l, c, k):
        for copy in second_hop(k):
            copy.wait()
        slot = k % 2
        B3[...] = (O1[...] + R2[slot, 0].astype(F32) + R2[slot, 1].astype(F32) + R2[slot, 2].astype(F32)).astype(BF16)
        O2[...] = O1[z] + R2[slot, 0, z].astype(F32) + R2[slot, 1, z].astype(F32) + R2[slot, 2, z].astype(F32)
        for copy in third_hop(k):
            copy.start()

    def stage_3(l, c, k):
        for copy in third_hop(k):
            copy.wait()

        @pl.when(k > 0)
        def _():
            before = k - 1
            wait_fourth(1 - before // chunks, before % chunks)

        slot = k % 2
        total = O2[...]
        for j in range(3):
            total = total + R3[slot, j].astype(F32)
        total = total.astype(BF16)
        B4[...] = total
        OGU[l, :, pl.ds(pl.multiple_of(z * 16, 16), 16), columns(c)] = total[0:2]
        p = S * c + s

        @pl.when(p // chunks == s)
        def _():
            rows, cols = place_d(p, z)
            OD[l, rows, cols] = total[2]

        for copy in spread_gu(l, c):
            copy.start()
        each_d(c, lambda zz: spread_d(l, c, zz).start())

    def layer(li, _):
        l = 1 - li

        def chunk(c, _):
            k = li * chunks + c
            cs = columns(c)

            @pl.when(li == 0)
            def _():
                arrived(1, GU, c)

            @pl.when(li == 0)
            def _():
                for t in range(tiles // 2):
                    r = pl.ds(t * 2 * tile, 2 * tile)
                    a = A[r, :]
                    g, u = dot(a, WG[1, :, cs], NN), dot(a, WU[1, :, cs], NN)
                    dz = dot(DH[r, :], WD[1, cs, :], NT).astype(BF16).astype(F32)
                    gate = 1.0 / (1.0 + jnp.exp(-g))
                    act = g * gate
                    Z[r, :] = (act * u).astype(BF16)
                    DU[r, cs] = (dz * act).astype(BF16)
                    DG[r, cs] = (dz * (u * (gate + act * (1.0 - gate)))).astype(BF16)

            @pl.when(li == 1)
            def _():
                for t in range(tiles):
                    factors_in(c, t).wait()
                for t in range(tiles // 2):
                    r = pl.ds(t * 2 * tile, 2 * tile)
                    dz = dot(DH[r, :], WD[0, cs, :], NT).astype(BF16).astype(F32)
                    DU[r, cs] = (dz * F[0, r]).astype(BF16)
                    DG[r, cs] = (dz * F[1, r]).astype(BF16)
                hidden_in(c).wait()

                @pl.when(c < chunks - 1)
                def _():
                    for t in range(tiles):
                        factors_in(c + 1, t).start()

            @pl.when(jnp.logical_and(li == 0, c < chunks - 1))
            def _():
                forward(1, GU, c + 1)

            for back, stage in ((3, stage_3), (2, stage_2), (1, stage_1)):
                @pl.when(c >= back)
                def _(back=back, stage=stage):
                    stage(l, c - back, k - back)

            by_gate = dot(AT[...], DG[:, cs], NN).astype(BF16)
            by_up = dot(AT[...], DU[:, cs], NN).astype(BF16)
            by_down = dot(Z[...], DH[...], ((0,), (0,))).astype(BF16)
            for dev in range(S):
                for q in range(R):
                    to_block = C.at[dev % 2, dev // 2, q]
                    top = rows_d * dev + 16 * q
                    to_block[0] = by_gate[top:top + 16]
                    to_block[1] = by_up[top:top + 16]
                    top = 32 * dev + 16 * (q // 2)
                    to_block[2] = by_down[top:top + 16, (q % 2) * W:(q % 2) * W + W]
            first_hop(k).start()

            @pl.when(jnp.logical_and(li == 1, c < chunks - 1))
            def _():
                hidden_in(c + 1).start()

            return 0

        lax.fori_loop(0, chunks, chunk, 0)

        @pl.when(li == 0)
        def _():
            pltpu.make_async_copy(keep_a, A, keep_sem.at[0]).start()
            pltpu.make_async_copy(keep_at, AT, keep_sem.at[1]).start()
            hidden_in(0).start()
            for t in range(tiles):
                factors_in(0, t).start()

        def below(i, _):
            r = pl.ds(pl.multiple_of(i * small, small), small)
            for q in range(2):
                r2 = pl.ds(pl.multiple_of(i * small + q * fine, fine), fine)
                da = (dot(DG[r2, :], WG[l], NT).astype(BF16).astype(F32)
                      + dot(DU[r2, :], WU[l], NT).astype(BF16).astype(F32)).astype(BF16).astype(F32)
                wide = H[r2, :].astype(F32)
                scale = lax.rsqrt(mean_square(wide))
                along = jnp.mean(da * wide, axis=-1, keepdims=True)
                by_h = (scale * da - wide * (scale * scale * scale * along)).astype(BF16)
                DH[r2, :] = (by_h.astype(F32) + DH[r2, :].astype(F32)).astype(BF16)

            @pl.when(li == 0)
            def _():
                pltpu.make_async_copy(x_ref.at[0, r], H.at[r], in_sem.at[0, i]).start()

            @pl.when(li == 1)
            def _():
                pltpu.make_async_copy(DH.at[r], dx_ref.at[0, r], dx_sem.at[i]).start()

            k = li * chunks + chunks - 1
            for step, stage, back in ((0, stage_3, 2), (0, stage_2, 1), (0, stage_1, 0), (3, stage_3, 1), (3, stage_2, 0), (5, stage_3, 0)):
                @pl.when(i == step * few // 8)
                def _(stage=stage, back=back):
                    stage(l, chunks - 1 - back, k - back)

            return 0

        lax.fori_loop(0, few, below, 0)

        @pl.when(li == 0)
        def _():
            pltpu.make_async_copy(keep_a, A, keep_sem.at[0]).wait()
            pltpu.make_async_copy(keep_at, AT, keep_sem.at[1]).wait()
            for i in range(few):
                x_in(i)[0].wait()

        return 0

    lax.fori_loop(0, 2, layer, 0)

    wait_fourth(0, chunks - 1)
    for l in range(2):
        for c in range(chunks):
            for copy in spread_gu(l, c):
                copy.wait_recv()
        for pos in range(chunks):
            p = s * chunks + pos
            for zz in range(R):
                @pl.when(jnp.logical_not(jnp.logical_and(p % S == s, z == zz)))
                def _(l=l, pos=pos, zz=zz):
                    rows, cols = place_d(pos, zz)
                    to(s4_sem.at[0], rd_sem.at[l, pos, zz], B4.at[2], OD.at[l, rows, cols], z, s).wait_recv()
    last = (pltpu.make_async_copy(OGU.at[:, 0], og_ref, out_sem.at[0]),
            pltpu.make_async_copy(OGU.at[:, 1], ou_ref, out_sem.at[1]),
            pltpu.make_async_copy(OD, od_ref, out_sem.at[2]))
    for copy in last:
        copy.start()
    for l in range(2):
        sent(l, DOWN, 0)

        def all_sent(c, _, l=l):
            sent(l, GU, c)
            return 0

        lax.fori_loop(0, chunks, all_sent, 0)
    for i in range(few):
        r = pl.ds(i * small, small)
        pltpu.make_async_copy(DH.at[r], dx_ref.at[0, r], dx_sem.at[i]).wait()
    for copy in last:
        copy.wait()


def whole(tokens, d, ff):
    tile, small = min(1024, tokens // 4), min(512, tokens // 8)
    few = tokens // small
    chunks = ff // W
    dma = pltpu.SemaphoreType.DMA
    layers = 2
    shape = jax.ShapeDtypeStruct
    rows_d, rows_f = d // S, ff // S
    any_space = pl.BlockSpec(memory_space=pl.ANY)
    flops = 2 * tokens * d * ff * 17
    return pl.pallas_call(
        functools.partial(kernel, tokens, d, ff, tile, small),
        out_shape=(
            shape((1, tokens, d), BF16), shape((layers, rows_d, ff), BF16), shape((layers, rows_d, ff), BF16),
            shape((layers, rows_f, d), BF16), shape((tokens, d), BF16), shape((d, tokens), BF16),
            shape((chunks, 2, tokens, W), F32), shape((tokens, ff), BF16)),
        in_specs=[any_space] * 5,
        out_specs=(any_space,) * 8,
        scratch_shapes=[
            pltpu.VMEM((layers, d, ff), BF16), pltpu.VMEM((layers, d, ff), BF16), pltpu.VMEM((layers, ff, d), BF16),
            pltpu.VMEM((tokens, d), BF16), pltpu.VMEM((d, tokens), BF16),
            pltpu.VMEM((tokens, d), BF16), pltpu.VMEM((tokens, d), BF16),
            pltpu.VMEM((tokens, ff), BF16), pltpu.VMEM((tokens, ff), BF16),
            pltpu.VMEM((tokens, W), BF16), pltpu.VMEM((2, tokens, W), F32),
            pltpu.VMEM((2, 4, R, 3, 16, W), BF16), pltpu.VMEM((2, 4, R, 3, 16, W), BF16),
            pltpu.VMEM((R, 3, 16, W), F32), pltpu.VMEM((4, R, 3, 16, W), BF16),
            pltpu.VMEM((2, 3, R, 3, 16, W), BF16), pltpu.VMEM((3, 16, W), F32),
            pltpu.VMEM((R, 3, 16, W), BF16), pltpu.VMEM((2, 3, 3, 16, W), BF16),
            pltpu.VMEM((3, 16, W), BF16),
            pltpu.VMEM((layers, 2, rows_d, ff), BF16), pltpu.VMEM((layers, rows_f, d), BF16),
            dma((2, few)), dma((layers, 3)), dma((2,)),
            dma((layers, 3, chunks, 4)), dma((layers, 3, chunks, 4)), dma((layers, 3, chunks, 3)), dma((layers, 3, chunks, 3)),
            dma((1,)), dma((2,)), dma((3,)), dma((2, 3)), dma((3,)), dma((2, 3)),
            dma((7,)), dma((layers, chunks, 3)), dma((layers, chunks, R)), dma((3,)), dma((few,)), dma((tokens // tile,)), dma((1,)),
        ],
        compiler_params=pltpu.CompilerParams(has_side_effects=True, collective_id=0, vmem_limit_bytes=67_043_328),
        cost_estimate=pl.CostEstimate(flops=flops, bytes_accessed=4 * tokens * d * 2, transcendentals=0),
        name="stack",
    )


def hand_on(*refs):
    n = len(refs) // 4
    ins, outs, held, (sems,) = refs[:4], refs[4:8], refs[8:12], refs[12:]
    parts = [(0, slice(512 * i, 512 * (i + 1))) for i in range(ins[0].shape[1] // 512)]
    jobs = [(0, part) for part in parts] + [(i, (slice(None),)) for i in range(1, n + 3) if i < 4]
    copies = []
    for q, (i, (*lead, rows)) in enumerate(jobs):
        at = (*lead, pl.ds(rows.start, 512)) if rows.start is not None else (pl.ds(0, ins[i].shape[0]),)
        copies.append((pltpu.make_async_copy(ins[i].at[at], held[i].at[at], sems.at[0, q]),
                       pltpu.make_async_copy(held[i].at[at], outs[i].at[at], sems.at[1, q])))
    for into, _ in copies:
        into.start()
    for into, out in copies:
        into.wait()
        out.start()
    for _, out in copies:
        out.wait()


def handed_on(*arrays):
    any_space = pl.BlockSpec(memory_space=pl.ANY)
    jobs = arrays[0].shape[1] // 512 + 3
    return pl.pallas_call(
        hand_on,
        out_shape=tuple(jax.ShapeDtypeStruct(a.shape, a.dtype) for a in arrays),
        in_specs=[any_space] * 4,
        out_specs=(any_space,) * 4,
        scratch_shapes=[pltpu.VMEM(a.shape, a.dtype) for a in arrays] + [pltpu.SemaphoreType.DMA((2, jobs))],
        name="hand_on",
    )(*arrays)


def solution(mesh):
    def step(x, dy, w_gate, w_up, w_down):
        _, tokens, d = x.shape
        ff = w_gate.shape[2]
        return handed_on(*whole(tokens, d, ff)(x, dy, w_gate, w_up, w_down)[:4])

    states, cut = P(("rep", "r", "s"), None, None), P(None, "s", None)
    return jax.shard_map(
        step,
        mesh=mesh,
        in_specs=(states, states) + (cut,) * 3,
        out_specs=(states,) + (P("rep", "s", None),) * 3,
        check_vma=False,
    )
```
